32 devices in a mesh: part: 1 (over z), data: 4 (over y), stage: 8 (over x, core).
Axes of the slice: x: 4, y: 4, z: 1, core: 2. Of those that a mesh axis runs over, the one named last changes fastest.
The devices are a block of a 4x4x8 slice.
Arguments:
- x: bfloat16 [32, 256, 768], P(('part', 'data'))
- g: bfloat16 [32, 256, 768], P(('part', 'data'))
- w_in: bfloat16 [2, 8, 768, 3072], P(None, 'stage')
- w_out: bfloat16 [2, 8, 3072, 768], P(None, 'stage')
Outputs:
- output 1: bfloat16 [32, 256, 768], P(('part', 'data'))
- output 2: bfloat16 [32, 256, 768], P(('part', 'data'))
- output 3: float32 [2, 8, 768, 3072], P('part', 'stage')
- output 4: float32 [2, 8, 3072, 768], P('part', 'stage')
All inputs are finite; a program needn't handle non-finite values.
Results may differ from the reference program's by a relative error of at most 0.02.
Values are sent between devices in bfloat16 or wider.
A program may use at most 768 MiB of HBM per device.

```python
import functools
import jax
import jax.numpy as jnp
from jax import lax

D_MODEL = 768
D_FF = 3072
MICRO_TOKENS = 256
ROUNDS = 1
DEVICE_LAYERS = 2
DATA_SIZE = 4
STAGE_SIZE = 8
MICRO_COUNT = ROUNDS * DATA_SIZE * STAGE_SIZE
LAYER_COUNT = DEVICE_LAYERS * STAGE_SIZE


def setup_inputs(seed: int = 0, part: int = 0) -> dict:
    base_key = jax.random.key(seed)
    shared_key, local_key = jax.random.split(base_key)
    local_key = jax.random.fold_in(local_key, part)
    key_in, key_out = jax.random.split(shared_key)
    key_x, key_g = jax.random.split(local_key)
    out_scale = D_FF ** -0.5 * min(0.5, (2.0 / LAYER_COUNT) ** 0.5)
    w_first = jax.random.normal(key_in, (DEVICE_LAYERS, STAGE_SIZE, D_MODEL, D_FF), jnp.float32) * D_MODEL ** -0.5
    w_second = jax.random.normal(key_out, (DEVICE_LAYERS, STAGE_SIZE, D_FF, D_MODEL), jnp.float32) * out_scale
    x_draw = jax.random.normal(key_x, (MICRO_COUNT, MICRO_TOKENS, D_MODEL), jnp.float32)
    g_draw = jax.random.normal(key_g, (MICRO_COUNT, MICRO_TOKENS, D_MODEL), jnp.float32)
    return {'x': x_draw.astype(jnp.bfloat16), 'g': g_draw.astype(jnp.bfloat16), 'w_in': w_first.astype(jnp.bfloat16), 'w_out': w_second.astype(jnp.bfloat16)}


def layer_forward(h_in, w_first, w_second):
    pre_act = jnp.dot(h_in, w_first, preferred_element_type=jnp.float32)
    hidden = jax.nn.gelu(pre_act, approximate=True).astype(jnp.bfloat16)
    delta_out = jnp.dot(hidden, w_second, preferred_element_type=jnp.float32)
    return (h_in.astype(jnp.float32) + delta_out).astype(jnp.bfloat16)


def layer_backward(h_in, w_first, w_second, g_next):
    pre_act = jnp.dot(h_in, w_first, preferred_element_type=jnp.float32)
    gelu_val, gelu_pull = jax.vjp(functools.partial(jax.nn.gelu, approximate=True), pre_act)
    hidden = gelu_val.astype(jnp.bfloat16)
    grad_second = jnp.dot(hidden.T, g_next, preferred_element_type=jnp.float32)
    grad_hidden = jnp.dot(g_next, w_second.T, preferred_element_type=jnp.float32)
    grad_pre = gelu_pull(grad_hidden)[0].astype(jnp.bfloat16)
    grad_first = jnp.dot(h_in.T, grad_pre, preferred_element_type=jnp.float32)
    grad_prev = jnp.dot(grad_pre, w_first.T, preferred_element_type=jnp.float32)
    g_prev = (g_next.astype(jnp.float32) + grad_prev).astype(jnp.bfloat16)
    return g_prev, grad_first, grad_second


def reference(x, g, w_in, w_out):
    first_all = w_in.reshape(LAYER_COUNT, D_MODEL, D_FF)
    second_all = w_out.reshape(LAYER_COUNT, D_FF, D_MODEL)

    def forward_step(h_cur, weights):
        return layer_forward(h_cur, weights[0], weights[1]), h_cur

    def backward_step(g_next, layer_items):
        h_cur, w_first, w_second, acc_first, acc_second = layer_items
        g_prev, grad_first, grad_second = layer_backward(h_cur, w_first, w_second, g_next)
        return g_prev, (acc_first + grad_first, acc_second + grad_second)

    def per_micro(accums, mb_pair):
        x_micro, g_micro = mb_pair
        y_micro, h_saved = lax.scan(forward_step, x_micro, (first_all, second_all))
        dx_micro, new_accums = lax.scan(backward_step, g_micro, (h_saved, first_all, second_all, accums[0], accums[1]), reverse=True)
        return new_accums, (y_micro, dx_micro)

    zero_first = jnp.zeros((LAYER_COUNT, D_MODEL, D_FF), jnp.float32)
    zero_second = jnp.zeros((LAYER_COUNT, D_FF, D_MODEL), jnp.float32)
    accums, results = lax.scan(per_micro, (zero_first, zero_second), (x, g))
    return (results[0], results[1], accums[0].reshape(DEVICE_LAYERS, STAGE_SIZE, D_MODEL, D_FF), accums[1].reshape(DEVICE_LAYERS, STAGE_SIZE, D_FF, D_MODEL))
```

```python
import functools
import jax
import jax.numpy as jnp
from jax import lax
from jax.experimental import pallas as pl
from jax.experimental.pallas import tpu as pltpu
from jax.sharding import PartitionSpec as P

MESH = pl.DeviceIdType.MESH
F32 = jnp.float32
BF16 = jnp.bfloat16
ANY = pl.BlockSpec(memory_space=pl.ANY)
GELU_A = 0.7978845608028654
GELU_B = 0.044715
VMEM_LIMIT = 66_000_000


def dot(a, b):
    return jnp.dot(a, b, preferred_element_type=F32)


def dot_tn(a, b):
    return lax.dot_general(a, b, (((0,), (0,)), ((), ())), preferred_element_type=F32)


def pick_block(size, target):
    block = min(size, target)
    while size % block:
        block //= 2
    return block


def stage_barrier(stages, levels, all_levels):
    s = lax.axis_index('stage')
    sem = pltpu.get_barrier_semaphore()
    count = 0
    for step in range(1, stages):
        pl.semaphore_signal(sem, inc=1, device_id={'stage': lax.rem(s + step, stages)}, device_id_type=MESH)
        count += 1
    if all_levels:
        d = lax.axis_index('data')
        for step in range(1, levels):
            pl.semaphore_signal(sem, inc=1, device_id={'data': lax.rem(d + step, levels)}, device_id_type=MESH)
            count += 1
    pl.semaphore_wait(sem, count)


def fwd_kernel(stages, levels, vees, micros, chunks, x_ref, wi_hbm, wo_hbm, *refs):
    h_outs, (y_out, wi, wo, hbuf, obuf, abuf, w_sem, x_sem, h_sem, y_sem, send_sem, recv_sem) = refs[:vees], refs[vees:]
    s = lax.axis_index('stage')
    nxt = lax.rem(s + 1, stages)
    _, dim, hid = wi.shape
    units = vees * micros
    fb = pick_block(hid, 512)
    nb = dim // chunks
    first = s == 0
    last = s == stages - 1

    def w_copies(v):
        return (pltpu.make_async_copy(wi_hbm.at[v], wi.at[v], w_sem.at[v, 0]),
                pltpu.make_async_copy(wo_hbm.at[v], wo.at[v], w_sem.at[v, 1]))

    def x_copy(m):
        return pltpu.make_async_copy(x_ref.at[m], hbuf.at[m], x_sem.at[m])

    def send(i, c, slot):
        cols = slice(c * nb, (c + 1) * nb)
        return pltpu.make_async_remote_copy(
            src_ref=obuf.at[i, :, cols], dst_ref=hbuf.at[slot, :, cols], send_sem=send_sem.at[i], recv_sem=recv_sem.at[slot],
            device_id={'stage': nxt}, device_id_type=MESH)

    def whole(i, slot):
        return pltpu.make_async_remote_copy(
            src_ref=obuf.at[i], dst_ref=hbuf.at[slot], send_sem=send_sem.at[i], recv_sem=recv_sem.at[slot],
            device_id={'stage': nxt}, device_id_type=MESH)

    def save(i, v):
        return pltpu.make_async_copy(hbuf.at[i], h_outs[v].at[i - v * micros], h_sem.at[i])

    for v in range(vees):
        for c in w_copies(v):
            c.start()

    @pl.when(first)
    def _():
        lax.fori_loop(0, micros, lambda m, _: (x_copy(m).start(), 0)[1], 0)

    stage_barrier(stages, levels, False)

    def unit(i, v):
        slot = jnp.where(last, i + micros, i)
        local_in = first & (v == 0)
        final = last & (v == vees - 1)

        @pl.when(local_in)
        def _():
            x_copy(i).wait()

        @pl.when(jnp.logical_not(local_in))
        def _():
            whole(i, i).wait_recv()

        save(i, v).start()
        for f in range(hid // fb):
            cols = slice(f * fb, (f + 1) * fb)
            z = dot(hbuf[i], wi[v, :, cols])
            t = jnp.tanh(GELU_A * (z + GELU_B * (z * z * z)))
            abuf[:, cols] = (z * (0.5 * (1.0 + t))).astype(BF16)
        for c in range(chunks):
            cols = slice(c * nb, (c + 1) * nb)
            out = hbuf[i, :, cols].astype(F32) + dot(abuf[...], wo[v, :, cols])
            obuf[i, :, cols] = out.astype(BF16)

            @pl.when(jnp.logical_not(final))
            def _():
                send(i, c, slot).start()

        @pl.when(final)
        def _():
            pltpu.make_async_copy(obuf.at[i], y_out.at[i - (vees - 1) * micros], y_sem.at[i - (vees - 1) * micros]).start()

    for v in range(vees):
        for c in w_copies(v):
            c.wait()

        def body(m, _, v=v):
            unit(v * micros + m, v)
            return 0
        lax.fori_loop(0, micros, body, 0)

    def drain(i, v):
        save(i, v).wait()
        final = last & (v == vees - 1)

        @pl.when(jnp.logical_not(final))
        def _():
            whole(i, i).wait_send()

        @pl.when(final)
        def _():
            pltpu.make_async_copy(obuf.at[i], y_out.at[i - (vees - 1) * micros], y_sem.at[i - (vees - 1) * micros]).wait()

    for v in range(vees):
        def tail(m, _, v=v):
            drain(v * micros + m, v)
            return 0
        lax.fori_loop(0, micros, tail, 0)


def run_fwd(stages, levels, x, w_in, w_out):
    micros, tokens, dim = x.shape
    vees, _, hid = w_in.shape
    units = vees * micros
    chunks = 3 if dim % 384 == 0 else 1
    flops = units * 4 * tokens * dim * hid
    return pl.pallas_call(
        functools.partial(fwd_kernel, stages, levels, vees, micros, chunks),
        out_shape=(jax.ShapeDtypeStruct((micros, tokens, dim), BF16),) * (vees + 1),
        in_specs=[ANY] * 3, out_specs=(ANY,) * (vees + 1),
        scratch_shapes=[
            pltpu.VMEM((vees, dim, hid), BF16), pltpu.VMEM((vees, hid, dim), BF16),
            pltpu.VMEM((units, tokens, dim), BF16), pltpu.VMEM((units, tokens, dim), BF16), pltpu.VMEM((tokens, hid), BF16),
            pltpu.SemaphoreType.DMA((vees, 2)), pltpu.SemaphoreType.DMA((micros,)), pltpu.SemaphoreType.DMA((units,)),
            pltpu.SemaphoreType.DMA((micros,)), pltpu.SemaphoreType.DMA((units,)), pltpu.SemaphoreType.DMA((units,)),
        ],
        compiler_params=pltpu.CompilerParams(collective_id=0, has_side_effects=True, vmem_limit_bytes=VMEM_LIMIT),
        cost_estimate=pl.CostEstimate(flops=flops, bytes_accessed=2 * units * tokens * dim * 2, transcendentals=units * tokens * hid),
        name='fwd_pipe',
    )(x, w_in, w_out)


def bwd_kernel(stages, levels, micros, groups, chunks, v, *refs):
    wide = groups > 1
    if wide:
        (h_hbm, e_hbm, _, wi_hbm, wo_hbm, gin_hbm, gout_hbm, dx_out, y_out, wi, wit, wot, tmp, gin, gout, ebuf, hbuf, obuf, abuf, qbuf,
         w_sem, t_sem, h_sem, l_sem, g_sem, send_sem, recv_sem, relay_send, dx_sem, dx_send, dx_recv, y_send, y_recv) = refs
    else:
        (h_hbm, e_hbm, wi_hbm, wo_hbm, gin_hbm, gout_hbm, dx_out, wi, wit, wot, tmp, gin, gout, ebuf, hbuf, obuf, abuf, qbuf,
         w_sem, t_sem, h_sem, l_sem, g_sem, send_sem, recv_sem, dx_sem) = refs
    s = lax.axis_index('stage')
    d = lax.axis_index('data')
    prv = lax.rem(s + stages - 1, stages)
    dim, hid = wi.shape
    units = groups * micros
    fb = pick_block(hid, 512)
    nb = dim // chunks
    tb = tmp.shape[1]
    hslots = hbuf.shape[0]
    oslots = obuf.shape[0]
    first = s == 0
    last = s == stages - 1

    def row_of(i):
        if not wide:
            return i
        return lax.rem(d + i // micros, levels) * micros + lax.rem(i, micros)

    def h_copy(i):
        return pltpu.make_async_copy(h_hbm.at[row_of(i)], hbuf.at[lax.rem(i, hslots)], h_sem.at[lax.rem(i, hslots)])

    def e_copy(m):
        return pltpu.make_async_copy(e_hbm.at[m], ebuf.at[m], l_sem.at[m])

    def hop(i, c=None):
        o = lax.rem(i, oslots)
        if c is None:
            src, dst = obuf.at[o], ebuf.at[i]
        else:
            cols = slice(c * nb, (c + 1) * nb)
            src, dst = obuf.at[o, :, cols], ebuf.at[i, :, cols]
        return pltpu.make_async_remote_copy(src_ref=src, dst_ref=dst, send_sem=send_sem.at[o], recv_sem=recv_sem.at[i],
                                            device_id={'stage': prv}, device_id_type=MESH)

    def entry(m):
        return pltpu.make_async_remote_copy(src_ref=e_hbm.at[m], dst_ref=ebuf.at[m], send_sem=l_sem.at[m], recv_sem=recv_sem.at[m],
                                            device_id={'stage': prv}, device_id_type=MESH)

    def dx_copy(m):
        return pltpu.make_async_copy(obuf.at[m], dx_out.at[m], dx_sem.at[m])

    def relay(m, j):
        slot = (levels - j) * micros + m
        return pltpu.make_async_remote_copy(src_ref=ebuf.at[m], dst_ref=ebuf.at[slot], send_sem=relay_send.at[m, j - 1],
                                            recv_sem=recv_sem.at[slot], device_id={'data': lax.rem(d + j, levels)}, device_id_type=MESH)

    def share(src, dst, send, recv, m, j):
        return pltpu.make_async_remote_copy(src_ref=src.at[m], dst_ref=dst.at[m], send_sem=send.at[m, j - 1], recv_sem=recv.at[m],
                                            device_id={'stage': lax.rem(s + j, stages)}, device_id_type=MESH)

    def loop(lo, hi, fn):
        def body(i, _):
            fn(i)
            return 0
        lax.fori_loop(lo, hi, body, 0)

    wi_copy = pltpu.make_async_copy(wi_hbm.at[v], wi, w_sem)
    wi_copy.start()

    def wo_copy(b):
        return pltpu.make_async_copy(wo_hbm.at[v, pl.ds(b * tb, tb)], tmp.at[b % 2], t_sem.at[b % 2])

    wo_copy(0).start()
    h_copy(0).start()
    gin[...] = jnp.zeros_like(gin)
    gout[...] = jnp.zeros_like(gout)
    wi_copy.wait()
    for b in range(hid // tb):
        rows = slice(b * tb, (b + 1) * tb)
        if b + 1 < hid // tb:
            wo_copy(b + 1).start()
        wit[rows, :] = wi[:, rows].T
        wo_copy(b).wait()
        wot[:, rows] = tmp[b % 2].T

    stage_barrier(stages, levels, wide)

    if wide:
        @pl.when(first)
        def _():
            loop(0, micros, lambda m: entry(m).start())
    else:
        @pl.when(last)
        def _():
            loop(0, micros, lambda m: e_copy(m).start())

    def unit(i):
        hs = lax.rem(i, hslots)
        o = lax.rem(i, oslots)
        h_copy(i).wait()

        @pl.when(i + 1 < units)
        def _():
            h_copy(i + 1).start()

        if wide:
            hop(i).wait_recv()

            @pl.when(last & (i < micros))
            def _():
                for j in range(1, levels):
                    relay(i, j).start()

            @pl.when(last & (i >= micros) & (i < 2 * micros))
            def _():
                m = i - micros
                for j in range(1, stages):
                    share(y_out, y_out, y_send, y_recv, m, j).start()
        else:
            @pl.when(last)
            def _():
                e_copy(i).wait()

            @pl.when(jnp.logical_not(last))
            def _():
                hop(i).wait_recv()

        for f in range(hid // fb):
            cols = slice(f * fb, (f + 1) * fb)
            z = dot(hbuf[hs], wi[:, cols])
            ga = dot(ebuf[i], wot[:, cols])
            z2 = z * z
            t = jnp.tanh(GELU_A * (z + GELU_B * (z2 * z)))
            cdf = 0.5 * (1.0 + t)
            slope = cdf + (0.5 * z) * (1.0 - t * t) * (GELU_A * (1.0 + (3.0 * GELU_B) * z2))
            abuf[:, cols] = (z * cdf).astype(BF16)
            qbuf[:, cols] = (slope * ga).astype(BF16)

        @pl.when(jnp.logical_not(first) & (i >= oslots))
        def _():
            hop(i - oslots).wait_send()

        @pl.when(jnp.logical_not(first) | (i < micros))
        def _():
            for c in range(chunks):
                cols = slice(c * nb, (c + 1) * nb)
                out = ebuf[i, :, cols].astype(F32) + dot(qbuf[...], wit[:, cols])
                obuf[o, :, cols] = out.astype(BF16)

                @pl.when(jnp.logical_not(first))
                def _():
                    hop(i, c).start()

        @pl.when(first & (i < micros))
        def _():
            dx_copy(i).start()
            if wide:
                for j in range(1, stages):
                    share(obuf, dx_out, dx_send, dx_recv, i, j).start()

        for f in range(hid // fb):
            cols = slice(f * fb, (f + 1) * fb)
            gin[:, cols] += dot_tn(hbuf[hs], qbuf[:, cols])
            gout[cols, :] += dot_tn(abuf[:, cols], ebuf[i])

    loop(0, units, unit)

    gin_copy = pltpu.make_async_copy(gin, gin_hbm, g_sem.at[0])
    gout_copy = pltpu.make_async_copy(gout, gout_hbm, g_sem.at[1])
    gin_copy.start()
    gout_copy.start()

    @pl.when(jnp.logical_not(first))
    def _():
        loop(units - oslots, units, lambda i: hop(i).wait_send())

    @pl.when(first)
    def _():
        loop(0, micros, lambda m: dx_copy(m).wait())

    if wide:
        @pl.when(first)
        def _():
            loop(0, micros, lambda m: entry(m).wait_send())
            for j in range(1, stages):
                loop(0, micros, lambda m, j=j: share(obuf, dx_out, dx_send, dx_recv, m, j).wait_send())

        @pl.when(last)
        def _():
            for j in range(1, levels):
                loop(0, micros, lambda m, j=j: relay(m, j).wait_send())
            for j in range(1, stages):
                loop(0, micros, lambda m, j=j: share(y_out, y_out, y_send, y_recv, m, j).wait_send())

        @pl.when(jnp.logical_not(first))
        def _():
            loop(0, micros, lambda m: share(obuf, dx_out, dx_send, dx_recv, m, 1).wait_recv())

        @pl.when(jnp.logical_not(last))
        def _():
            loop(0, micros, lambda m: share(y_out, y_out, y_send, y_recv, m, 1).wait_recv())

    gin_copy.wait()
    gout_copy.wait()


def run_bwd(stages, levels, v, h, e, y, wi, wo):
    micros, tokens, dim = e.shape
    hid = wi.shape[2]
    wide = y is not None
    groups = h.shape[0] // micros
    units = groups * micros
    chunks = 3 if dim % 384 == 0 else 1
    tb = pick_block(hid, 768)
    dma = pltpu.SemaphoreType.DMA
    small = jax.ShapeDtypeStruct((micros, tokens, dim), BF16)
    out_shape = [jax.ShapeDtypeStruct((dim, hid), F32), jax.ShapeDtypeStruct((hid, dim), F32), small]
    operands = [h, e]
    scratch = [
        pltpu.VMEM((dim, hid), BF16), pltpu.VMEM((hid, dim), BF16), pltpu.VMEM((dim, hid), BF16), pltpu.VMEM((2, tb, dim), BF16),
        pltpu.VMEM((dim, hid), F32), pltpu.VMEM((hid, dim), F32), pltpu.VMEM((units, tokens, dim), BF16),
        pltpu.VMEM((2, tokens, dim), BF16), pltpu.VMEM((micros, tokens, dim), BF16),
        pltpu.VMEM((tokens, hid), BF16), pltpu.VMEM((tokens, hid), BF16),
        dma, dma((2,)), dma((2,)), dma((micros,)), dma((2,)), dma((micros,)), dma((units,)),
    ]
    aliases = {}
    if wide:
        operands.append(y)
        out_shape.append(small)
        aliases = {2: 3}
        scratch += [dma((micros, levels - 1)), dma((micros,)), dma((micros, stages - 1)), dma((micros,)),
                    dma((micros, stages - 1)), dma((micros,))]
    else:
        scratch += [dma((micros,))]
    operands += [wi, wo]
    return pl.pallas_call(
        functools.partial(bwd_kernel, stages, levels, micros, groups, chunks, v),
        out_shape=tuple(out_shape), in_specs=[ANY] * len(operands), out_specs=(ANY,) * len(out_shape),
        scratch_shapes=scratch, input_output_aliases=aliases,
        compiler_params=pltpu.CompilerParams(collective_id=2 if wide else 1, has_side_effects=True, vmem_limit_bytes=VMEM_LIMIT),
        cost_estimate=pl.CostEstimate(flops=units * 10 * tokens * dim * hid, bytes_accessed=units * tokens * dim * 4,
                                      transcendentals=units * tokens * hid),
        name='bwd_wide' if wide else 'bwd_own',
    )(*operands)


def solution(mesh):
    stages, levels = mesh.shape['stage'], mesh.shape['data']

    def local_fn(x, g, w_in, w_out):
        wi, wo = w_in[:, 0], w_out[:, 0]
        h_lo, h_up, y = run_fwd(stages, levels, x, wi, wo)
        h_all = lax.all_gather(h_lo, 'data', axis=0, tiled=True)
        gin_up, gout_up, e_mid = run_bwd(stages, levels, 1, h_up, g, None, wi, wo)
        gin_up, gout_up = lax.psum((gin_up, gout_up), 'data')
        gin_lo, gout_lo, dx, y = run_bwd(stages, levels, 0, h_all, e_mid, y, wi, wo)
        grad_in = jnp.stack([gin_lo, gin_up])[:, None]
        grad_out = jnp.stack([gout_lo, gout_up])[:, None]
        return y, dx, grad_in, grad_out

    spec_rows = P(('part', 'data'))
    spec_weights = P(None, 'stage')
    spec_grads = P('part', 'stage')
    return jax.shard_map(local_fn, mesh=mesh, in_specs=(spec_rows, spec_rows, spec_weights, spec_weights), out_specs=(spec_rows, spec_rows, spec_grads, spec_grads), check_vma=False)
```

```python
import functools
import jax
import jax.numpy as jnp
from jax import lax
from jax.experimental import pallas as pl
from jax.experimental.pallas import tpu as pltpu
from jax.sharding import PartitionSpec as P

MESH = pl.DeviceIdType.MESH
F32 = jnp.float32
BF16 = jnp.bfloat16
ANY = pl.BlockSpec(memory_space=pl.ANY)
GELU_A = 0.7978845608028654
GELU_B = 0.044715
VMEM_LIMIT = 66_000_000


def dot(a, b):
    return jnp.dot(a, b, preferred_element_type=F32)


def dot_nt(a, b):
    return lax.dot_general(a, b, (((1,), (1,)), ((), ())), preferred_element_type=F32)


def dot_tn(a, b):
    return lax.dot_general(a, b, (((0,), (0,)), ((), ())), preferred_element_type=F32)


def gelu_only(z):
    t = jnp.tanh(z * (GELU_A + (GELU_A * GELU_B) * (z * z)))
    return z * (0.5 * t + 0.5)


def gelu_and_slope(z):
    s = (GELU_A * GELU_B) * (z * z)
    cdf = 0.5 * jnp.tanh(z * (GELU_A + s)) + 0.5
    a = z * cdf
    return a, cdf + (a * (1.0 - cdf)) * (2.0 * GELU_A + 6.0 * s)


def pick_block(size, target):
    block = min(size, target)
    while size % block:
        block //= 2
    return block


def loop(lo, hi, fn):
    def body(i, _):
        fn(i)
        return 0
    lax.fori_loop(lo, hi, body, 0)


def signal_all(targets):
    sem = pltpu.get_barrier_semaphore()
    for target in targets:
        pl.semaphore_signal(sem, inc=1, device_id=target, device_id_type=MESH)
    pl.semaphore_wait(sem, len(targets))


def slices(size, block):
    return [slice(b * block, (b + 1) * block) for b in range(size // block)]


def act_pass(h, wi, a, slope, fb):
    for cols in slices(wi.shape[1], fb):
        act, der = gelu_and_slope(dot(h[...], wi[:, cols]))
        a[:, cols] = act.astype(BF16)
        slope[:, cols] = der


def grad_pass(h, e, q, a, gin, gout, h_next, wi, a_next, slope, fb):
    for cols in slices(wi.shape[1], fb):
        gin[:, cols] += dot_tn(h[...], q[:, cols])
        gout[cols, :] += dot_tn(a[:, cols], e[...])
        act, der = gelu_and_slope(dot(h_next[...], wi[:, cols]))
        a_next[:, cols] = act.astype(BF16)
        slope[:, cols] = der


def front_kernel(stages, levels, micros, chunks, x_hbm, g_hbm, wi_hbm, wo_hbm, hall, y_out, eall, gin_hbm, gout_hbm,
                 wi, wo, hbuf, obuf, ebuf, gin, gout, abuf, qbuf, slope,
                 w_sem, x_sem, g_sem, f_send, f_recv, b_send, b_recv, y_sem, h_save, h_send, h_recv, e_save, e_send, e_recv, o_sem):
    s = lax.axis_index('stage')
    d = lax.axis_index('data')
    nxt, prv = lax.rem(s + 1, stages), lax.rem(s + stages - 1, stages)
    up, down = lax.rem(d + 1, levels), lax.rem(d + levels - 1, levels)
    _, dim, hid = wi.shape
    tokens = hbuf.shape[1]
    half = tokens // 2
    nb = dim // chunks
    fb = pick_block(hid, 768)
    first = s == 0
    last = s == stages - 1
    lag = jnp.minimum(3 * (stages - 1 - s) + 1, micros)

    def w_copies(v):
        return (pltpu.make_async_copy(wi_hbm.at[v], wi.at[v], w_sem.at[v, 0]),
                pltpu.make_async_copy(wo_hbm.at[v], wo.at[v], w_sem.at[v, 1]))

    def x_copy(m):
        return pltpu.make_async_copy(x_hbm.at[m], hbuf.at[m], x_sem.at[m])

    def g_copy(m):
        return pltpu.make_async_copy(g_hbm.at[m], ebuf.at[m], g_sem.at[m])

    def f_hop(i, slot, cols=slice(None)):
        return pltpu.make_async_remote_copy(
            src_ref=obuf.at[lax.rem(i, micros), :, cols], dst_ref=hbuf.at[slot, :, cols], send_sem=f_send.at[i], recv_sem=f_recv.at[slot],
            device_id={'stage': nxt}, device_id_type=MESH)

    def b_hop(m, cols=slice(None)):
        return pltpu.make_async_remote_copy(
            src_ref=obuf.at[m, :, cols], dst_ref=ebuf.at[m, :, cols], send_sem=b_send.at[m], recv_sem=b_recv.at[m],
            device_id={'stage': prv}, device_id_type=MESH)

    def y_copy(m):
        return pltpu.make_async_copy(obuf.at[m], y_out.at[m], y_sem.at[m])

    def h_keep(m):
        return pltpu.make_async_copy(hbuf.at[m], hall.at[m], h_save.at[m])

    def h_push(m, j):
        return pltpu.make_async_remote_copy(
            src_ref=hbuf.at[m], dst_ref=hall.at[(2 - j) * micros + m], send_sem=h_send.at[j, m], recv_sem=h_recv.at[1 - j, m],
            device_id={'data': (up, down)[j]}, device_id_type=MESH)

    def h_forward(m, j):
        rows = (slice(0, half), slice(half, tokens))[j]
        return pltpu.make_async_remote_copy(
            src_ref=hall.at[(2 - j) * micros + m, rows], dst_ref=hall.at[3 * micros + m, rows], send_sem=h_send.at[2 + j, m],
            recv_sem=h_recv.at[2, m], device_id={'data': (up, down)[j]}, device_id_type=MESH)

    def h_whole(m):
        return pltpu.make_async_remote_copy(
            src_ref=hall.at[m], dst_ref=hall.at[3 * micros + m], send_sem=h_send.at[2, m], recv_sem=h_recv.at[2, m],
            device_id={'data': up}, device_id_type=MESH)

    def e_keep(m):
        return pltpu.make_async_copy(obuf.at[m], eall.at[m], e_save.at[m])

    def e_push(m, j):
        return pltpu.make_async_remote_copy(
            src_ref=obuf.at[m], dst_ref=eall.at[(2 - j) * micros + m], send_sem=e_send.at[j, m], recv_sem=e_recv.at[1 - j, m],
            device_id={'data': (up, down)[j]}, device_id_type=MESH)

    for v in range(2):
        for c in w_copies(v):
            c.start()

    @pl.when(first)
    def _():
        loop(0, micros, lambda m: x_copy(m).start())

    @pl.when(last)
    def _():
        loop(0, micros, lambda m: g_copy(m).start())

    signal_all([{'stage': lax.rem(s + step, stages)} for step in range(1, stages)] + [{'data': up}, {'data': down}])

    for c in w_copies(0):
        c.wait()

    def fwd_unit(i, a):
        v = i // micros
        lower = i < micros
        o = lax.rem(i, micros)
        slot = jnp.where(last, i + micros, i)
        final = last & jnp.logical_not(lower)

        @pl.when(first & lower)
        def _():
            x_copy(i).wait()

        @pl.when(jnp.logical_not(first & lower))
        def _():
            f_hop(i, i).wait_recv()

        @pl.when(lower)
        def _():
            h_keep(i).start()
            h_push(i, 0).start()
            h_push(i, 1).start()

        @pl.when(jnp.logical_not(lower))
        def _():
            f_hop(o, o).wait_send()
            h_push(o, 0).wait_recv()
            h_push(o, 1).wait_recv()
            h_forward(o, 0).start()
            h_forward(o, 1).start()

        for cols in slices(hid, fb):
            a[:, cols] = gelu_only(dot(hbuf[i], wi[v, :, cols])).astype(BF16)
        for cols in slices(dim, nb):
            out = hbuf[i, :, cols].astype(F32) + dot(a[...], wo[v, :, cols])
            obuf[o, :, cols] = out.astype(BF16)

            @pl.when(jnp.logical_not(final))
            def _():
                f_hop(i, slot, cols).start()

        @pl.when(final)
        def _():
            y_copy(o).start()

    def bwd_unit(m):
        a, a_next = abuf.at[lax.rem(m, 2)], abuf.at[lax.rem(m + 1, 2)]
        h, h_next = hbuf.at[micros + m], hbuf.at[micros + jnp.minimum(m + 1, micros - 1)]

        @pl.when(last)
        def _():
            g_copy(m).wait()
            y_copy(m).wait()

        @pl.when(jnp.logical_not(last))
        def _():
            b_hop(m).wait_recv()
            f_hop(micros + m, micros + m).wait_send()

        for cols in slices(hid, fb):
            qbuf[:, cols] = (slope[:, cols] * dot_nt(ebuf[m], wo[1, cols, :])).astype(BF16)
        for cols in slices(dim, nb):
            out = ebuf[m, :, cols].astype(F32) + dot_nt(qbuf[...], wi[1, cols, :])
            obuf[m, :, cols] = out.astype(BF16)

            @pl.when(jnp.logical_not(first))
            def _():
                b_hop(m, cols).start()

        @pl.when(first)
        def _():
            e_keep(m).start()
            e_push(m, 0).start()
            e_push(m, 1).start()

        grad_pass(h, ebuf.at[m], qbuf, a, gin, gout, h_next, wi.at[1], a_next, slope, fb)

    def step(t):
        m = t - micros - lag

        @pl.when(t == micros)
        def _():
            gin[...] = jnp.zeros_like(gin)
            gout[...] = jnp.zeros_like(gout)
            for c in w_copies(1):
                c.wait()

        @pl.when(t < 2 * micros)
        def _():
            fwd_unit(t, abuf.at[lax.rem(t + lag + micros + 1, 2)])

        @pl.when(m == -1)
        def _():
            act_pass(hbuf.at[micros], wi.at[1], abuf.at[0], slope, fb)

        @pl.when((m >= 0) & (m < micros))
        def _():
            bwd_unit(m)

    loop(0, 2 * micros + lag, step)

    outs = (pltpu.make_async_copy(gin, gin_hbm, o_sem.at[0]), pltpu.make_async_copy(gout, gout_hbm, o_sem.at[1]))
    for c in outs:
        c.start()

    def drain(m):
        h_keep(m).wait()
        h_push(m, 0).wait_send()
        h_push(m, 1).wait_send()
        h_forward(m, 0).wait_send()
        h_forward(m, 1).wait_send()
        h_whole(m).wait_recv()

        @pl.when(jnp.logical_not(first))
        def _():
            b_hop(m).wait_send()

        @pl.when(first)
        def _():
            e_keep(m).wait()
            for j in range(2):
                e_push(m, j).wait_send()
                e_push(m, j).wait_recv()

    loop(0, micros, drain)
    for c in outs:
        c.wait()


def run_front(stages, levels, x, g, w_in, w_out):
    micros, tokens, dim = x.shape
    _, _, hid = w_in.shape
    chunks = 3 if dim % 384 == 0 else 1
    dma = pltpu.SemaphoreType.DMA

    def rows(n):
        return jax.ShapeDtypeStruct((n * micros, tokens, dim), BF16)

    return pl.pallas_call(
        functools.partial(front_kernel, stages, levels, micros, chunks),
        out_shape=(rows(4), rows(1), rows(3), jax.ShapeDtypeStruct((dim, hid), F32), jax.ShapeDtypeStruct((hid, dim), F32)),
        in_specs=[ANY] * 4, out_specs=(ANY,) * 5,
        scratch_shapes=[
            pltpu.VMEM((2, dim, hid), BF16), pltpu.VMEM((2, hid, dim), BF16),
            pltpu.VMEM((2 * micros, tokens, dim), BF16), pltpu.VMEM((micros, tokens, dim), BF16), pltpu.VMEM((micros, tokens, dim), BF16),
            pltpu.VMEM((dim, hid), F32), pltpu.VMEM((hid, dim), F32),
            pltpu.VMEM((2, tokens, hid), BF16), pltpu.VMEM((tokens, hid), BF16), pltpu.VMEM((tokens, hid), F32),
            dma((2, 2)), dma((micros,)), dma((micros,)), dma((2 * micros,)), dma((2 * micros,)), dma((micros,)), dma((micros,)), dma((micros,)),
            dma((micros,)), dma((4, micros)), dma((3, micros)), dma((micros,)), dma((2, micros)), dma((2, micros)), dma((2,)),
        ],
        compiler_params=pltpu.CompilerParams(collective_id=0, has_side_effects=True, vmem_limit_bytes=VMEM_LIMIT),
        cost_estimate=pl.CostEstimate(flops=micros * 18 * tokens * dim * hid, bytes_accessed=8 * micros * tokens * dim * 2,
                                      transcendentals=3 * micros * tokens * hid),
        name='front',
    )(x, g, w_in, w_out)


def wide_kernel(stages, levels, micros, chunks, hall, eall, _, wi_hbm, wo_hbm, gin_hbm, gout_hbm, dx_out, y_out,
                wi, wo, hbuf, obuf, ebuf, gin, gout, abuf, qbuf, slope,
                w_sem, h_sem, n_send, b_send, b_recv, dx_sem, dx_send, dx_recv, y_send, y_recv, o_sem):
    s = lax.axis_index('stage')
    d = lax.axis_index('data')
    nxt, prv = lax.rem(s + 1, stages), lax.rem(s + stages - 1, stages)
    up, down = lax.rem(d + 1, levels), lax.rem(d + levels - 1, levels)
    dim, hid = wi.shape
    tokens = hbuf.shape[1]
    half = tokens // 2
    units = ebuf.shape[0]
    nb = dim // chunks
    fb = pick_block(hid, 768)
    hslots = hbuf.shape[0]
    first = s == 0
    last = s == stages - 1

    w_copies = (pltpu.make_async_copy(wi_hbm.at[0], wi, w_sem.at[0]), pltpu.make_async_copy(wo_hbm.at[0], wo, w_sem.at[1]))

    def h_copy(i):
        return pltpu.make_async_copy(hall.at[i], hbuf.at[lax.rem(i, hslots)], h_sem.at[lax.rem(i, hslots)])

    def entry(i):
        return pltpu.make_async_remote_copy(
            src_ref=eall.at[i], dst_ref=ebuf.at[i], send_sem=n_send.at[i], recv_sem=b_recv.at[i],
            device_id={'stage': prv}, device_id_type=MESH)

    def entry_far(m, j):
        rows = (slice(0, half), slice(half, tokens))[j]
        return pltpu.make_async_remote_copy(
            src_ref=eall.at[(2 - j) * micros + m, rows], dst_ref=ebuf.at[3 * micros + m, rows], send_sem=n_send.at[(3 + j) * micros + m],
            recv_sem=b_recv.at[3 * micros + m], device_id={'stage': prv, 'data': (up, down)[j]}, device_id_type=MESH)

    def b_hop(i, cols=slice(None)):
        o = lax.rem(i, micros)
        return pltpu.make_async_remote_copy(
            src_ref=obuf.at[o, :, cols], dst_ref=ebuf.at[i, :, cols], send_sem=b_send.at[o], recv_sem=b_recv.at[i],
            device_id={'stage': prv}, device_id_type=MESH)

    def dx_copy(m):
        return pltpu.make_async_copy(obuf.at[m], dx_out.at[m], dx_sem.at[m])

    def share(src, dst, send, recv, m, j):
        return pltpu.make_async_remote_copy(
            src_ref=src.at[m], dst_ref=dst.at[m], send_sem=send.at[m, j - 1], recv_sem=recv.at[m],
            device_id={'stage': lax.rem(s + j, stages)}, device_id_type=MESH)

    for c in w_copies:
        c.start()
    for i in range(hslots - 1):
        h_copy(i).start()

    signal_all([{'stage': lax.rem(s + step, stages)} for step in range(1, stages)]
               + [{'stage': st, 'data': lv} for st in (nxt, prv) for lv in (up, down)])

    @pl.when(first)
    def _():
        loop(0, 3 * micros, lambda i: entry(i).start())
        loop(0, micros, lambda m: entry_far(m, 0).start())
        loop(0, micros, lambda m: entry_far(m, 1).start())

    gin[...] = jnp.zeros_like(gin)
    gout[...] = jnp.zeros_like(gout)
    for c in w_copies:
        c.wait()
    h_copy(0).wait()
    act_pass(hbuf.at[0], wi, abuf.at[0], slope, fb)

    def unit(i):
        a, a_next = abuf.at[lax.rem(i, 2)], abuf.at[lax.rem(i + 1, 2)]
        h, h_next = hbuf.at[lax.rem(i, hslots)], hbuf.at[lax.rem(jnp.minimum(i + 1, units - 1), hslots)]
        o = lax.rem(i, micros)

        @pl.when(i + hslots - 1 < units)
        def _():
            h_copy(i + hslots - 1).start()

        b_hop(i).wait_recv()

        @pl.when(last & (i >= micros) & (i < 2 * micros))
        def _():
            for j in range(1, stages):
                share(y_out, y_out, y_send, y_recv, i - micros, j).start()

        @pl.when(jnp.logical_not(first) & (i >= micros))
        def _():
            b_hop(i - micros).wait_send()

        for cols in slices(hid, fb):
            qbuf[:, cols] = (slope[:, cols] * dot_nt(ebuf[i], wo[cols, :])).astype(BF16)

        @pl.when(jnp.logical_not(first) | (i < micros))
        def _():
            for cols in slices(dim, nb):
                out = ebuf[i, :, cols].astype(F32) + dot_nt(qbuf[...], wi[cols, :])
                obuf[o, :, cols] = out.astype(BF16)

                @pl.when(jnp.logical_not(first))
                def _():
                    b_hop(i, cols).start()

        @pl.when(first & (i < micros))
        def _():
            dx_copy(i).start()
            for j in range(1, stages):
                share(obuf, dx_out, dx_send, dx_recv, i, j).start()

        @pl.when(i + 1 < units)
        def _():
            h_copy(i + 1).wait()

        grad_pass(h, ebuf.at[i], qbuf, a, gin, gout, h_next, wi, a_next, slope, pick_block(hid, 256))

    loop(0, units, unit)

    outs = (pltpu.make_async_copy(gin, gin_hbm, o_sem.at[0]), pltpu.make_async_copy(gout, gout_hbm, o_sem.at[1]))
    for c in outs:
        c.start()

    @pl.when(first)
    def _():
        loop(0, 3 * micros, lambda i: entry(i).wait_send())
        loop(0, micros, lambda m: entry_far(m, 0).wait_send())
        loop(0, micros, lambda m: entry_far(m, 1).wait_send())
        loop(0, micros, lambda m: dx_copy(m).wait())
        for j in range(1, stages):
            loop(0, micros, lambda m, j=j: share(obuf, dx_out, dx_send, dx_recv, m, j).wait_send())

    @pl.when(jnp.logical_not(first))
    def _():
        loop(units - micros, units, lambda i: b_hop(i).wait_send())
        loop(0, micros, lambda m: share(obuf, dx_out, dx_send, dx_recv, m, 1).wait_recv())

    @pl.when(last)
    def _():
        for j in range(1, stages):
            loop(0, micros, lambda m, j=j: share(y_out, y_out, y_send, y_recv, m, j).wait_send())

    @pl.when(jnp.logical_not(last))
    def _():
        loop(0, micros, lambda m: share(y_out, y_out, y_send, y_recv, m, 1).wait_recv())

    for c in outs:
        c.wait()


def run_wide(stages, levels, micros, hall, eall, y, w_in, w_out):
    units, tokens, dim = hall.shape
    _, _, hid = w_in.shape
    chunks = 3 if dim % 384 == 0 else 1
    dma = pltpu.SemaphoreType.DMA
    small = jax.ShapeDtypeStruct((micros, tokens, dim), BF16)
    return pl.pallas_call(
        functools.partial(wide_kernel, stages, levels, micros, chunks),
        out_shape=(jax.ShapeDtypeStruct((dim, hid), F32), jax.ShapeDtypeStruct((hid, dim), F32), small, small),
        in_specs=[ANY] * 5, out_specs=(ANY,) * 4,
        scratch_shapes=[
            pltpu.VMEM((dim, hid), BF16), pltpu.VMEM((hid, dim), BF16),
            pltpu.VMEM((4, tokens, dim), BF16), pltpu.VMEM((micros, tokens, dim), BF16), pltpu.VMEM((units, tokens, dim), BF16),
            pltpu.VMEM((dim, hid), F32), pltpu.VMEM((hid, dim), F32),
            pltpu.VMEM((2, tokens, hid), BF16), pltpu.VMEM((tokens, hid), BF16), pltpu.VMEM((tokens, hid), F32),
            dma((2,)), dma((4,)), dma((5 * micros,)), dma((micros,)), dma((units,)), dma((micros,)), dma((micros, stages - 1)), dma((micros,)),
            dma((micros, stages - 1)), dma((micros,)), dma((2,)),
        ],
        input_output_aliases={2: 3},
        compiler_params=pltpu.CompilerParams(collective_id=1, has_side_effects=True, vmem_limit_bytes=VMEM_LIMIT),
        cost_estimate=pl.CostEstimate(flops=units * 10 * tokens * dim * hid, bytes_accessed=units * tokens * dim * 4,
                                      transcendentals=units * tokens * hid),
        name='wide',
    )(hall, eall, y, w_in, w_out)


def place_kernel(gin, gout, dx, y, gin_out, gout_out, dx_out, y_out):
    gin_out[0] = gin[...]
    gout_out[0] = gout[...]
    dx_out[...] = dx[...]
    y_out[...] = y[...]


def run_place(gin, gout, dx, y):
    dim, hid = gin.shape
    micros, tokens, _ = dx.shape
    small = pl.BlockSpec((1, tokens, dim), lambda i: (i, 0, 0))
    return pl.pallas_call(
        place_kernel, grid=(micros,),
        out_shape=(jax.ShapeDtypeStruct((2, dim, hid), F32), jax.ShapeDtypeStruct((2, hid, dim), F32),
                   jax.ShapeDtypeStruct(dx.shape, BF16), jax.ShapeDtypeStruct(y.shape, BF16)),
        in_specs=[pl.BlockSpec((dim // micros, hid), lambda i: (i, 0)), pl.BlockSpec((hid // micros, dim), lambda i: (i, 0)), small, small],
        out_specs=(pl.BlockSpec((1, dim // micros, hid), lambda i: (0, i, 0)), pl.BlockSpec((1, hid // micros, dim), lambda i: (0, i, 0)),
                   small, small),
        cost_estimate=pl.CostEstimate(flops=dim * hid, bytes_accessed=16 * dim * hid, transcendentals=0),
        name='place',
    )(gin, gout, dx, y)


def solution(mesh):
    stages, levels = mesh.shape['stage'], mesh.shape['data']

    def local_fn(x, g, w_in, w_out):
        wi, wo = w_in[:, 0], w_out[:, 0]
        hall, y, eall, gin_up, gout_up = run_front(stages, levels, x, g, wi, wo)
        gin_up, gout_up = lax.psum((gin_up, gout_up), 'data')
        gin_lo, gout_lo, dx, y = run_wide(stages, levels, x.shape[0], hall, eall, y, wi, wo)
        grad_in, grad_out, dx, y = run_place(gin_lo, gout_lo, dx, y)
        grad_in = lax.dynamic_update_slice(grad_in, gin_up[None], (1, 0, 0))
        grad_out = lax.dynamic_update_slice(grad_out, gout_up[None], (1, 0, 0))
        return y, dx, grad_in[:, None], grad_out[:, None]

    spec_rows = P(('part', 'data'))
    spec_weights = P(None, 'stage')
    spec_grads = P('part', 'stage')
    return jax.shard_map(local_fn, mesh=mesh, in_specs=(spec_rows, spec_rows, spec_weights, spec_weights), out_specs=(spec_rows, spec_rows, spec_grads, spec_grads), check_vma=False)
```

```python
import functools
import jax
import jax.numpy as jnp
from jax import lax
from jax.experimental import pallas as pl
from jax.experimental.pallas import tpu as pltpu
from jax.sharding import PartitionSpec as P

MESH = pl.DeviceIdType.MESH
F32 = jnp.float32
BF16 = jnp.bfloat16
ANY = pl.BlockSpec(memory_space=pl.ANY)
GELU_A = 0.7978845608028654
GELU_B = 0.044715
VMEM_LIMIT = 66_000_000


def dot(a, b):
    return jnp.dot(a, b, preferred_element_type=F32)


def dot_nt(a, b):
    return lax.dot_general(a, b, (((1,), (1,)), ((), ())), preferred_element_type=F32)


def dot_tn(a, b):
    return lax.dot_general(a, b, (((0,), (0,)), ((), ())), preferred_element_type=F32)


def gelu_only(z):
    t = jnp.tanh(z * (GELU_A + (GELU_A * GELU_B) * (z * z)))
    return z * (0.5 * t + 0.5)


def gelu_and_slope(z):
    s = (GELU_A * GELU_B) * (z * z)
    cdf = 0.5 * jnp.tanh(z * (GELU_A + s)) + 0.5
    a = z * cdf
    return a, cdf + (a * (1.0 - cdf)) * (2.0 * GELU_A + 6.0 * s)


def pick_block(size, target):
    block = min(size, target)
    while size % block:
        block //= 2
    return block


def loop(lo, hi, fn):
    def body(i, _):
        fn(i)
        return 0
    lax.fori_loop(lo, hi, body, 0)


def signal_all(targets):
    sem = pltpu.get_barrier_semaphore()
    for target in targets:
        pl.semaphore_signal(sem, inc=1, device_id=target, device_id_type=MESH)
    pl.semaphore_wait(sem, len(targets))


def slices(size, block):
    return [slice(b * block, (b + 1) * block) for b in range(size // block)]


def act_pass(h, wi, a, slope, fb):
    for cols in slices(wi.shape[1], fb):
        act, der = gelu_and_slope(dot(h[...], wi[:, cols]))
        a[:, cols] = act.astype(BF16)
        slope[:, cols] = der


def front_kernel(stages, levels, micros, chunks, x_hbm, g_hbm, wi_hbm, wo_hbm, hall, y_out, eall, gin_hbm, gout_hbm, aup, qup,
                 wi, wo, hbuf, obuf, ebuf, gin, gout, abuf, qbuf, slope,
                 w_sem, x_sem, g_sem, f_send, f_recv, b_send, b_recv, y_sem, h_save, h_send, h_recv, e_save, e_send, e_recv,
                 a_save, a_load, o_sem):
    s = lax.axis_index('stage')
    d = lax.axis_index('data')
    nxt, prv = lax.rem(s + 1, stages), lax.rem(s + stages - 1, stages)
    up, down = lax.rem(d + 1, levels), lax.rem(d + levels - 1, levels)
    _, dim, hid = wi.shape
    tokens = hbuf.shape[1]
    half = tokens // 2
    nb = dim // chunks
    fb = pick_block(hid, 768)
    wb = pick_block(hid, 512)
    first = s == 0
    last = s == stages - 1
    inner = jnp.logical_not(last)
    lag = jnp.minimum(3 * (stages - 1 - s), micros)
    defer = s >= stages - 2

    def w_copies(v):
        return (pltpu.make_async_copy(wi_hbm.at[v], wi.at[v], w_sem.at[v, 0]),
                pltpu.make_async_copy(wo_hbm.at[v], wo.at[v], w_sem.at[v, 1]))

    def x_copy(m):
        return pltpu.make_async_copy(x_hbm.at[m], hbuf.at[m], x_sem.at[m])

    def g_copy(m):
        return pltpu.make_async_copy(g_hbm.at[m], ebuf.at[m], g_sem.at[m])

    def f_hop(i, slot, cols=slice(None)):
        return pltpu.make_async_remote_copy(
            src_ref=obuf.at[lax.rem(i, micros), :, cols], dst_ref=hbuf.at[slot, :, cols], send_sem=f_send.at[i], recv_sem=f_recv.at[slot],
            device_id={'stage': nxt}, device_id_type=MESH)

    def b_hop(m, cols=slice(None)):
        return pltpu.make_async_remote_copy(
            src_ref=obuf.at[m, :, cols], dst_ref=ebuf.at[m, :, cols], send_sem=b_send.at[m], recv_sem=b_recv.at[m],
            device_id={'stage': prv}, device_id_type=MESH)

    def y_copy(m):
        return pltpu.make_async_copy(obuf.at[m], y_out.at[m], y_sem.at[m])

    def h_keep(m):
        return pltpu.make_async_copy(hbuf.at[m], hall.at[m], h_save.at[m])

    def h_push(m, j):
        return pltpu.make_async_remote_copy(
            src_ref=hbuf.at[m], dst_ref=hall.at[(2 - j) * micros + m], send_sem=h_send.at[j, m], recv_sem=h_recv.at[1 - j, m],
            device_id={'data': (up, down)[j]}, device_id_type=MESH)

    def h_forward(m, j):
        rows = (slice(0, half), slice(half, tokens))[j]
        return pltpu.make_async_remote_copy(
            src_ref=hall.at[(2 - j) * micros + m, rows], dst_ref=hall.at[3 * micros + m, rows], send_sem=h_send.at[2 + j, m],
            recv_sem=h_recv.at[2, m], device_id={'data': (up, down)[j]}, device_id_type=MESH)

    def h_whole(m):
        return pltpu.make_async_remote_copy(
            src_ref=hall.at[m], dst_ref=hall.at[3 * micros + m], send_sem=h_send.at[2, m], recv_sem=h_recv.at[2, m],
            device_id={'data': up}, device_id_type=MESH)

    def e_keep(m):
        return pltpu.make_async_copy(obuf.at[m], eall.at[m], e_save.at[m])

    def e_push(m, j, cols=slice(None)):
        return pltpu.make_async_remote_copy(
            src_ref=obuf.at[m, :, cols], dst_ref=eall.at[(2 - j) * micros + m, :, cols], send_sem=e_send.at[j, m], recv_sem=e_recv.at[1 - j, m],
            device_id={'data': (up, down)[j]}, device_id_type=MESH)

    def e_forward(m, j):
        rows = (slice(0, half), slice(half, tokens))[j]
        return pltpu.make_async_remote_copy(
            src_ref=eall.at[(2 - j) * micros + m, rows], dst_ref=eall.at[3 * micros + m, rows], send_sem=e_send.at[2 + j, m],
            recv_sem=e_recv.at[2, m], device_id={'data': (up, down)[j]}, device_id_type=MESH)

    def e_whole(m):
        return pltpu.make_async_remote_copy(
            src_ref=eall.at[m], dst_ref=eall.at[3 * micros + m], send_sem=e_send.at[2, m], recv_sem=e_recv.at[2, m],
            device_id={'data': up}, device_id_type=MESH)

    def a_keep(m):
        return pltpu.make_async_copy(abuf.at[lax.rem(m, 2)], aup.at[m], a_save.at[0, m])

    def q_keep(m):
        return pltpu.make_async_copy(qbuf.at[lax.rem(m, 2)], qup.at[m], a_save.at[1, m])

    def loads(m):
        k = lax.rem(m, 2)
        return (pltpu.make_async_copy(aup.at[m], abuf.at[k], a_load.at[0, k]), pltpu.make_async_copy(qup.at[m], qbuf.at[k], a_load.at[1, k]))

    for v in range(2):
        for c in w_copies(v):
            c.start()

    @pl.when(first)
    def _():
        loop(0, micros, lambda m: x_copy(m).start())

    @pl.when(last)
    def _():
        loop(0, micros, lambda m: g_copy(m).start())

    signal_all([{'stage': lax.rem(s + step, stages)} for step in range(1, stages)] + [{'data': up}, {'data': down}])

    for c in w_copies(0):
        c.wait()

    def fwd_wait(i):
        lower = i < micros

        @pl.when(first & lower)
        def _():
            x_copy(i).wait()

        @pl.when(jnp.logical_not(first & lower))
        def _():
            f_hop(i, i).wait_recv()

    def fwd_unit(i, aslot):
        v = i // micros
        lower = i < micros
        upper = jnp.logical_not(lower)
        o = lax.rem(i, micros)
        slot = jnp.where(last, i + micros, i)
        final = last & upper
        a = abuf.at[aslot]

        @pl.when(lower)
        def _():
            h_keep(i).start()
            h_push(i, 0).start()
            h_push(i, 1).start()

        @pl.when(upper)
        def _():
            f_hop(o, o).wait_send()
            h_push(o, 0).wait_recv()
            h_push(o, 1).wait_recv()
            h_forward(o, 0).start()
            h_forward(o, 1).start()

        @pl.when(jnp.logical_not(final))
        def _():
            for cols in slices(hid, fb):
                a[:, cols] = gelu_only(dot(hbuf[i], wi[v, :, cols])).astype(BF16)

        for cols in slices(dim, nb):
            out = hbuf[i, :, cols].astype(F32) + dot(a[...], wo[v, :, cols])
            obuf[o, :, cols] = out.astype(BF16)

            @pl.when(jnp.logical_not(final))
            def _():
                f_hop(i, slot, cols).start()

        @pl.when(final)
        def _():
            y_copy(o).start()

    def bwd_unit(m):
        q = qbuf.at[lax.rem(m, 2)]

        @pl.when(last)
        def _():
            g_copy(m).wait()
            y_copy(m).wait()

        @pl.when(inner)
        def _():
            b_hop(m).wait_recv()
            f_hop(micros + m, micros + m).wait_send()

        @pl.when(defer & (m >= 2))
        def _():
            q_keep(m - 2).wait()

        for cols in slices(hid, fb):
            q[:, cols] = (slope[:, cols] * dot_nt(ebuf[m], wo[1, cols, :])).astype(BF16)
        for cols in slices(dim, nb):
            out = ebuf[m, :, cols].astype(F32) + dot_nt(q[...], wi[1, cols, :])
            obuf[m, :, cols] = out.astype(BF16)

            @pl.when(jnp.logical_not(first))
            def _():
                b_hop(m, cols).start()

            @pl.when(first)
            def _():
                e_push(m, 0, cols).start()
                e_push(m, 1, cols).start()

        @pl.when(first)
        def _():
            e_keep(m).start()

            @pl.when(m >= 1)
            def _():
                far(m - 1)

        @pl.when(defer)
        def _():
            q_keep(m).start()

    def far(m):
        for j in range(2):
            e_push(m, j).wait_recv()
        for j in range(2):
            e_forward(m, j).start()

    def weight_unit(m):
        k = lax.rem(m, 2)
        for cols in slices(hid, wb):
            gin[:, cols] += dot_tn(hbuf[micros + m], qbuf[k, :, cols])
            gout[cols, :] += dot_tn(abuf[k, :, cols], ebuf[m])

    def step(t):
        m = t - micros - lag
        active = (m >= 0) & (m < micros)
        put_off = m - micros
        w = jnp.where(defer, put_off, m)

        @pl.when(t == micros)
        def _():
            gin[...] = jnp.zeros_like(gin)
            gout[...] = jnp.zeros_like(gout)
            for c in w_copies(1):
                c.wait()

        early = last & active

        @pl.when(early)
        def _():
            fwd_wait(t)

        @pl.when(active)
        def _():
            @pl.when(defer & (m >= 2))
            def _():
                a_keep(m - 2).wait()

            act_pass(hbuf.at[micros + m], wi.at[1], abuf.at[lax.rem(m, 2)], slope, fb)

            @pl.when(defer)
            def _():
                a_keep(m).start()

        @pl.when(t < 2 * micros)
        def _():
            @pl.when(jnp.logical_not(early))
            def _():
                fwd_wait(t)

            fwd_unit(t, jnp.where(early, lax.rem(t + micros, 2), 2))

        @pl.when(active)
        def _():
            bwd_unit(m)

        @pl.when(put_off == 0)
        def _():
            for n in range(micros - 2, micros):
                a_keep(n).wait()
                q_keep(n).wait()
            for c in loads(0):
                c.start()

        @pl.when((put_off >= 0) & (put_off < micros - 1))
        def _():
            for c in loads(put_off + 1):
                c.start()

        @pl.when(put_off >= 0)
        def _():
            for c in loads(put_off):
                c.wait()

        @pl.when((w >= 0) & (w < micros))
        def _():
            weight_unit(w)

    loop(0, 2 * micros + lag + jnp.where(defer, micros, 0), step)

    outs = (pltpu.make_async_copy(gin, gin_hbm, o_sem.at[0]), pltpu.make_async_copy(gout, gout_hbm, o_sem.at[1]))
    for c in outs:
        c.start()

    @pl.when(first)
    def _():
        far(micros - 1)

    def drain(m):
        h_keep(m).wait()
        h_push(m, 0).wait_send()
        h_push(m, 1).wait_send()
        h_forward(m, 0).wait_send()
        h_forward(m, 1).wait_send()
        h_whole(m).wait_recv()

        @pl.when(jnp.logical_not(first))
        def _():
            b_hop(m).wait_send()

        @pl.when(first)
        def _():
            e_keep(m).wait()
            for j in range(2):
                e_push(m, j).wait_send()
                e_forward(m, j).wait_send()
            e_whole(m).wait_recv()

    loop(0, micros, drain)
    for c in outs:
        c.wait()


def run_front(stages, levels, x, g, w_in, w_out):
    micros, tokens, dim = x.shape
    _, _, hid = w_in.shape
    chunks = 3 if dim % 384 == 0 else 1
    dma = pltpu.SemaphoreType.DMA

    def rows(n):
        return jax.ShapeDtypeStruct((n * micros, tokens, dim), BF16)

    acts = jax.ShapeDtypeStruct((micros, tokens, hid), BF16)
    return pl.pallas_call(
        functools.partial(front_kernel, stages, levels, micros, chunks),
        out_shape=(rows(4), rows(1), rows(4), jax.ShapeDtypeStruct((dim, hid), F32), jax.ShapeDtypeStruct((hid, dim), F32), acts, acts),
        in_specs=[ANY] * 4, out_specs=(ANY,) * 7,
        scratch_shapes=[
            pltpu.VMEM((2, dim, hid), BF16), pltpu.VMEM((2, hid, dim), BF16),
            pltpu.VMEM((2 * micros, tokens, dim), BF16), pltpu.VMEM((micros, tokens, dim), BF16), pltpu.VMEM((micros, tokens, dim), BF16),
            pltpu.VMEM((dim, hid), F32), pltpu.VMEM((hid, dim), F32),
            pltpu.VMEM((3, tokens, hid), BF16), pltpu.VMEM((2, tokens, hid), BF16), pltpu.VMEM((tokens, hid), F32),
            dma((2, 2)), dma((micros,)), dma((micros,)), dma((2 * micros,)), dma((2 * micros,)), dma((micros,)), dma((micros,)), dma((micros,)),
            dma((micros,)), dma((4, micros)), dma((3, micros)), dma((micros,)), dma((4, micros)), dma((3, micros)),
            dma((2, micros)), dma((2, 2)), dma((2,)),
        ],
        compiler_params=pltpu.CompilerParams(collective_id=0, has_side_effects=True, vmem_limit_bytes=VMEM_LIMIT),
        cost_estimate=pl.CostEstimate(flops=micros * 18 * tokens * dim * hid, bytes_accessed=4 * micros * tokens * hid * 2,
                                      transcendentals=3 * micros * tokens * hid),
        name='front',
    )(x, g, w_in, w_out)


def wide_kernel(stages, micros, chunks, hall, eall, _, wi_hbm, wo_hbm, a_out, q_out, e_out, dx_out, y_out,
                wi, wo, hbuf, obuf, ebuf, abuf, qbuf,
                w_sem, h_sem, n_send, b_send, b_recv, dx_sem, dx_send, dx_recv, y_send, y_recv, s_sem):
    s = lax.axis_index('stage')
    nxt, prv = lax.rem(s + 1, stages), lax.rem(s + stages - 1, stages)
    dim, hid = wi.shape
    units = ebuf.shape[0]
    nb = dim // chunks
    fb = pick_block(hid, 768)
    hslots = hbuf.shape[0]
    first = s == 0
    last = s == stages - 1

    w_copies = (pltpu.make_async_copy(wi_hbm.at[0], wi, w_sem.at[0]), pltpu.make_async_copy(wo_hbm.at[0], wo, w_sem.at[1]))

    def h_copy(i):
        return pltpu.make_async_copy(hall.at[i], hbuf.at[lax.rem(i, hslots)], h_sem.at[lax.rem(i, hslots)])

    def entry(i):
        return pltpu.make_async_remote_copy(
            src_ref=eall.at[i], dst_ref=ebuf.at[i], send_sem=n_send.at[i], recv_sem=b_recv.at[i],
            device_id={'stage': prv}, device_id_type=MESH)

    def b_hop(i, cols=slice(None)):
        o = lax.rem(i, micros)
        return pltpu.make_async_remote_copy(
            src_ref=obuf.at[o, :, cols], dst_ref=ebuf.at[i, :, cols], send_sem=b_send.at[o], recv_sem=b_recv.at[i],
            device_id={'stage': prv}, device_id_type=MESH)

    def dx_copy(m):
        return pltpu.make_async_copy(obuf.at[m], dx_out.at[m], dx_sem.at[m])

    def dx_hop(m, src):
        return pltpu.make_async_remote_copy(
            src_ref=src.at[m], dst_ref=dx_out.at[m], send_sem=dx_send.at[m], recv_sem=dx_recv.at[m],
            device_id={'stage': nxt}, device_id_type=MESH)

    def y_hop(m):
        return pltpu.make_async_remote_copy(
            src_ref=y_out.at[m], dst_ref=y_out.at[m], send_sem=y_send.at[m], recv_sem=y_recv.at[m],
            device_id={'stage': nxt}, device_id_type=MESH)

    def relay(i):
        my = jnp.where(last, i - 1, i - 2 - 3 * s)
        mx = i - 1 - 3 * s

        @pl.when((my >= 0) & (my < micros))
        def _():
            @pl.when(jnp.logical_not(last))
            def _():
                y_hop(my).wait_recv()

            @pl.when(s != stages - 2)
            def _():
                y_hop(my).start()

        @pl.when((mx >= 0) & (mx < micros) & jnp.logical_not(first))
        def _():
            dx_hop(mx, dx_out).wait_recv()

            @pl.when(jnp.logical_not(last))
            def _():
                dx_hop(mx, dx_out).start()

    def keep(i):
        k = lax.rem(i, 2)
        return (pltpu.make_async_copy(abuf.at[k], a_out.at[i], s_sem.at[0, k]), pltpu.make_async_copy(qbuf.at[k], q_out.at[i], s_sem.at[1, k]),
                pltpu.make_async_copy(ebuf.at[i], e_out.at[i], s_sem.at[2, k]))

    for c in w_copies:
        c.start()
    for i in range(hslots - 1):
        h_copy(i).start()

    signal_all([{'stage': lax.rem(s + step, stages)} for step in range(1, stages)])

    @pl.when(first)
    def _():
        loop(0, units, lambda i: entry(i).start())

    for c in w_copies:
        c.wait()

    def unit(i):
        k = lax.rem(i, 2)
        a, q, h = abuf.at[k], qbuf.at[k], hbuf.at[lax.rem(i, hslots)]
        o = lax.rem(i, micros)

        @pl.when(i + hslots - 1 < units)
        def _():
            h_copy(i + hslots - 1).start()

        h_copy(i).wait()
        b_hop(i).wait_recv()

        @pl.when(i >= 2)
        def _():
            for c in keep(i - 2):
                c.wait()

        relay(i)

        @pl.when(jnp.logical_not(first) & (i >= micros))
        def _():
            b_hop(i - micros).wait_send()

        for cols in slices(hid, fb):
            act, der = gelu_and_slope(dot(h[...], wi[:, cols]))
            a[:, cols] = act.astype(BF16)
            q[:, cols] = (der * dot_nt(ebuf[i], wo[cols, :])).astype(BF16)

        @pl.when(jnp.logical_not(first) | (i < micros))
        def _():
            for cols in slices(dim, nb):
                out = ebuf[i, :, cols].astype(F32) + dot_nt(q[...], wi[cols, :])
                obuf[o, :, cols] = out.astype(BF16)

                @pl.when(jnp.logical_not(first))
                def _():
                    b_hop(i, cols).start()

        @pl.when(first & (i < micros))
        def _():
            dx_copy(i).start()
            dx_hop(i, obuf).start()

        for c in keep(i):
            c.start()

    loop(0, units, unit)
    loop(units, max(units, micros + 3 * stages - 2), relay)

    @pl.when(first)
    def _():
        loop(0, units, lambda i: entry(i).wait_send())
        loop(0, micros, lambda m: dx_copy(m).wait())

    @pl.when(jnp.logical_not(first))
    def _():
        loop(units - micros, units, lambda i: b_hop(i).wait_send())

    @pl.when(jnp.logical_not(last))
    def _():
        loop(0, micros, lambda m: dx_hop(m, dx_out).wait_send())

    @pl.when(s != stages - 2)
    def _():
        loop(0, micros, lambda m: y_hop(m).wait_send())

    for i in (units - 2, units - 1):
        for c in keep(i):
            c.wait()


def run_wide(stages, micros, hall, eall, y, w_in, w_out):
    units, tokens, dim = hall.shape
    _, _, hid = w_in.shape
    chunks = 3 if dim % 384 == 0 else 1
    dma = pltpu.SemaphoreType.DMA
    small = jax.ShapeDtypeStruct((micros, tokens, dim), BF16)
    acts = jax.ShapeDtypeStruct((units, tokens, hid), BF16)
    return pl.pallas_call(
        functools.partial(wide_kernel, stages, micros, chunks),
        out_shape=(acts, acts, jax.ShapeDtypeStruct((units, tokens, dim), BF16), small, small),
        in_specs=[ANY] * 5, out_specs=(ANY,) * 5,
        scratch_shapes=[
            pltpu.VMEM((dim, hid), BF16), pltpu.VMEM((hid, dim), BF16),
            pltpu.VMEM((4, tokens, dim), BF16), pltpu.VMEM((micros, tokens, dim), BF16), pltpu.VMEM((units, tokens, dim), BF16),
            pltpu.VMEM((2, tokens, hid), BF16), pltpu.VMEM((2, tokens, hid), BF16),
            dma((2,)), dma((4,)), dma((units,)), dma((micros,)), dma((units,)), dma((micros,)), dma((micros,)), dma((micros,)),
            dma((micros,)), dma((micros,)), dma((3, 2)),
        ],
        input_output_aliases={2: 4},
        compiler_params=pltpu.CompilerParams(collective_id=1, has_side_effects=True, vmem_limit_bytes=VMEM_LIMIT),
        cost_estimate=pl.CostEstimate(flops=units * 6 * tokens * dim * hid, bytes_accessed=units * tokens * hid * 4,
                                      transcendentals=units * tokens * hid),
        name='wide',
    )(hall, eall, y, w_in, w_out)


def wgrad_kernel(lhs, rhs, out):
    @pl.when(pl.program_id(1) == 0)
    def _():
        out[...] = jnp.zeros_like(out)

    out[0] += dot_tn(lhs[...], rhs[...])


def run_wgrad(lhs, rhs, split_lhs, name):
    lhs, rhs = lhs.reshape(-1, lhs.shape[-1]), rhs.reshape(-1, rhs.shape[-1])
    tokens, m, n = lhs.shape[0], lhs.shape[1], rhs.shape[1]
    kb = pick_block(tokens, 2048)
    fb = pick_block(m if split_lhs else n, 1024)
    if split_lhs:
        grid, block = (m // fb, tokens // kb), (1, fb, n)
        lhs_spec, rhs_spec = pl.BlockSpec((kb, fb), lambda j, k: (k, j)), pl.BlockSpec((kb, n), lambda j, k: (k, 0))
        place = lambda j, k: (0, j, 0)
    else:
        grid, block = (n // fb, tokens // kb), (1, m, fb)
        lhs_spec, rhs_spec = pl.BlockSpec((kb, m), lambda j, k: (k, 0)), pl.BlockSpec((kb, fb), lambda j, k: (k, j))
        place = lambda j, k: (0, 0, j)
    return pl.pallas_call(
        wgrad_kernel, grid=grid, out_shape=jax.ShapeDtypeStruct((2, m, n), F32), in_specs=[lhs_spec, rhs_spec],
        out_specs=pl.BlockSpec(block, place), compiler_params=pltpu.CompilerParams(vmem_limit_bytes=VMEM_LIMIT),
        cost_estimate=pl.CostEstimate(flops=2 * tokens * m * n, bytes_accessed=2 * tokens * (m + n) + 4 * m * n, transcendentals=0),
        name=name,
    )(lhs, rhs)


def place_kernel(dx, y, dx_out, y_out):
    dx_out[...] = dx[...]
    y_out[...] = y[...]


def run_place(dx, y):
    spec = pl.BlockSpec((1,) + dx.shape[1:], lambda i: (i, 0, 0))
    shape = jax.ShapeDtypeStruct(dx.shape, BF16)
    return pl.pallas_call(
        place_kernel, grid=(dx.shape[0],), out_shape=(shape, shape), in_specs=[spec] * 2, out_specs=(spec, spec),
        cost_estimate=pl.CostEstimate(flops=dx.size, bytes_accessed=8 * dx.size, transcendentals=0), name='place',
    )(dx, y)


def solution(mesh):
    stages, levels = mesh.shape['stage'], mesh.shape['data']

    def local_fn(x, g, w_in, w_out):
        wi, wo = w_in[:, 0], w_out[:, 0]
        hall, y, eall, gin_up, gout_up, _, _ = run_front(stages, levels, x, g, wi, wo)
        gin_up, gout_up = lax.psum((gin_up, gout_up), 'data')
        alow, qlow, elow, dx, y = run_wide(stages, x.shape[0], hall, eall, y, wi, wo)
        grad_in = run_wgrad(hall, qlow, False, 'gin_low')
        grad_out = run_wgrad(alow, elow, True, 'gout_low')
        dx, y = run_place(dx, y)
        grad_in = lax.dynamic_update_slice(grad_in, gin_up[None], (1, 0, 0))
        grad_out = lax.dynamic_update_slice(grad_out, gout_up[None], (1, 0, 0))
        return y, dx, grad_in[:, None], grad_out[:, None]

    spec_rows = P(('part', 'data'))
    spec_weights = P(None, 'stage')
    spec_grads = P('part', 'stage')
    return jax.shard_map(local_fn, mesh=mesh, in_specs=(spec_rows, spec_rows, spec_weights, spec_weights), out_specs=(spec_rows, spec_rows, spec_grads, spec_grads), check_vma=False)
```

```python
import functools
import jax
import jax.numpy as jnp
from jax import lax
from jax.experimental import pallas as pl
from jax.experimental.pallas import tpu as pltpu
from jax.sharding import PartitionSpec as P

MESH = pl.DeviceIdType.MESH
F32 = jnp.float32
BF16 = jnp.bfloat16
ANY = pl.BlockSpec(memory_space=pl.ANY)
GELU_A = 0.7978845608028654
GELU_B = 0.044715
VMEM_LIMIT = 67_043_328


def dot(a, b):
    return jnp.dot(a, b, preferred_element_type=F32)


def dot_nt(a, b):
    return lax.dot_general(a, b, (((1,), (1,)), ((), ())), preferred_element_type=F32)


def dot_tn(a, b):
    return lax.dot_general(a, b, (((0,), (0,)), ((), ())), preferred_element_type=F32)


def gelu_only(z):
    t = jnp.tanh(z * (GELU_A + (GELU_A * GELU_B) * (z * z)))
    return z * (0.5 * t + 0.5)


def gelu_and_slope(z):
    s = (GELU_A * GELU_B) * (z * z)
    cdf = 0.5 * jnp.tanh(z * (GELU_A + s)) + 0.5
    a = z * cdf
    return a, cdf + (a * (1.0 - cdf)) * (2.0 * GELU_A + 6.0 * s)


def pick_block(size, target):
    block = min(size, target)
    while size % block:
        block //= 2
    return block


def loop(lo, hi, fn):
    def body(i, _):
        fn(i)
        return 0
    lax.fori_loop(lo, hi, body, 0)


def head_units(s, micros):
    return jnp.minimum(jnp.maximum(s - 1, 0), micros)


def head_arrivals(s, stages, micros):
    return jnp.where(s == stages - 1, micros, head_units(s + 1, micros))


def signal_all(targets):
    sem = pltpu.get_barrier_semaphore()
    for target in targets:
        pl.semaphore_signal(sem, inc=1, device_id=target, device_id_type=MESH)
    pl.semaphore_wait(sem, len(targets))


def slices(size, block):
    return [slice(b * block, (b + 1) * block) for b in range(size // block)]


def act_pass(h, wi, a, slope, fb):
    for cols in slices(wi.shape[1], fb):
        act, der = gelu_and_slope(dot(h[...], wi[:, cols]))
        a[:, cols] = act.astype(BF16)
        slope[:, cols] = der


def front_kernel(stages, levels, micros, chunks, x_hbm, g_hbm, wi_hbm, wo_hbm, hall, y_out, eall, gin_hbm, gout_hbm, aup, qup, alow, qlow, elow,
                 wi, wo, hbuf, obuf, ebuf, gin, gout, abuf, qbuf, slope,
                 w_sem, x_sem, g_sem, f_send, f_recv, b_send, b_recv, y_sem, h_save, h_send, h_recv, e_save, e_send, e_recv,
                 a_save, a_load, o_sem, l_save):
    s = lax.axis_index('stage')
    d = lax.axis_index('data')
    nxt, prv = lax.rem(s + 1, stages), lax.rem(s + stages - 1, stages)
    up, down = lax.rem(d + 1, levels), lax.rem(d + levels - 1, levels)
    _, dim, hid = wi.shape
    tokens = hbuf.shape[1]
    half = tokens // 2
    nb = dim // chunks
    fb = pick_block(hid, 768)
    wb = pick_block(hid, 512)
    first = s == 0
    last = s == stages - 1
    inner = jnp.logical_not(last)
    lag = jnp.minimum(3 * (stages - 1 - s), micros)
    defer = s >= stages - 2
    heads, arrivals = head_units(s, micros), head_arrivals(s, stages, micros)

    def w_copies(v):
        return (pltpu.make_async_copy(wi_hbm.at[v], wi.at[v], w_sem.at[v, 0]),
                pltpu.make_async_copy(wo_hbm.at[v], wo.at[v], w_sem.at[v, 1]))

    def x_copy(m):
        return pltpu.make_async_copy(x_hbm.at[m], hbuf.at[m], x_sem.at[m])

    def g_copy(m):
        return pltpu.make_async_copy(g_hbm.at[m], ebuf.at[m], g_sem.at[m])

    def f_hop(i, slot, cols=slice(None)):
        return pltpu.make_async_remote_copy(
            src_ref=obuf.at[lax.rem(i, micros), :, cols], dst_ref=hbuf.at[slot, :, cols], send_sem=f_send.at[i], recv_sem=f_recv.at[slot],
            device_id={'stage': nxt}, device_id_type=MESH)

    def b_hop(m, cols=slice(None)):
        return pltpu.make_async_remote_copy(
            src_ref=obuf.at[lax.rem(m, micros), :, cols], dst_ref=ebuf.at[m, :, cols], send_sem=b_send.at[m], recv_sem=b_recv.at[m],
            device_id={'stage': prv}, device_id_type=MESH)

    def entry(m, cols=slice(None)):
        return pltpu.make_async_remote_copy(
            src_ref=obuf.at[m, :, cols], dst_ref=ebuf.at[micros + m, :, cols], send_sem=b_send.at[m], recv_sem=b_recv.at[micros + m],
            device_id={'stage': prv}, device_id_type=MESH)

    def low_keep(k):
        return (pltpu.make_async_copy(abuf.at[0], alow.at[k], l_save.at[0]), pltpu.make_async_copy(qbuf.at[0], qlow.at[k], l_save.at[1]))

    def e_low_keep(k):
        return pltpu.make_async_copy(ebuf.at[micros + k], elow.at[k], l_save.at[2 + k])

    def y_copy(m):
        return pltpu.make_async_copy(obuf.at[m], y_out.at[m], y_sem.at[m])

    def h_keep(m):
        return pltpu.make_async_copy(hbuf.at[m], hall.at[m], h_save.at[m])

    def h_push(m, j):
        return pltpu.make_async_remote_copy(
            src_ref=hbuf.at[m], dst_ref=hall.at[(2 - j) * micros + m], send_sem=h_send.at[j, m], recv_sem=h_recv.at[1 - j, m],
            device_id={'data': (up, down)[j]}, device_id_type=MESH)

    def h_forward(m, j):
        rows = (slice(0, half), slice(half, tokens))[j]
        return pltpu.make_async_remote_copy(
            src_ref=hall.at[(2 - j) * micros + m, rows], dst_ref=hall.at[3 * micros + m, rows], send_sem=h_send.at[2 + j, m],
            recv_sem=h_recv.at[2, m], device_id={'data': (up, down)[j]}, device_id_type=MESH)

    def h_whole(m):
        return pltpu.make_async_remote_copy(
            src_ref=hall.at[m], dst_ref=hall.at[3 * micros + m], send_sem=h_send.at[2, m], recv_sem=h_recv.at[2, m],
            device_id={'data': up}, device_id_type=MESH)

    def e_keep(m):
        return pltpu.make_async_copy(obuf.at[m], eall.at[m], e_save.at[m])

    def e_push(m, j, cols=slice(None)):
        return pltpu.make_async_remote_copy(
            src_ref=obuf.at[m, :, cols], dst_ref=eall.at[(2 - j) * micros + m, :, cols], send_sem=e_send.at[j, m], recv_sem=e_recv.at[1 - j, m],
            device_id={'data': (up, down)[j]}, device_id_type=MESH)

    def e_forward(m, j):
        rows = (slice(0, half), slice(half, tokens))[j]
        return pltpu.make_async_remote_copy(
            src_ref=eall.at[(2 - j) * micros + m, rows], dst_ref=eall.at[3 * micros + m, rows], send_sem=e_send.at[2 + j, m],
            recv_sem=e_recv.at[2, m], device_id={'data': (up, down)[j]}, device_id_type=MESH)

    def e_whole(m):
        return pltpu.make_async_remote_copy(
            src_ref=eall.at[m], dst_ref=eall.at[3 * micros + m], send_sem=e_send.at[2, m], recv_sem=e_recv.at[2, m],
            device_id={'data': up}, device_id_type=MESH)

    def a_keep(m):
        return pltpu.make_async_copy(abuf.at[lax.rem(m, 2)], aup.at[m], a_save.at[0, m])

    def q_keep(m):
        return pltpu.make_async_copy(qbuf.at[lax.rem(m, 2)], qup.at[m], a_save.at[1, m])

    def loads(m):
        return (pltpu.make_async_copy(aup.at[m], abuf.at[1], a_load.at[0]), pltpu.make_async_copy(qup.at[m], qbuf.at[1], a_load.at[1]))

    for v in range(2):
        for c in w_copies(v):
            c.start()

    @pl.when(first)
    def _():
        loop(0, micros, lambda m: x_copy(m).start())

    @pl.when(last)
    def _():
        loop(0, micros, lambda m: g_copy(m).start())

    signal_all([{'stage': lax.rem(s + step, stages)} for step in range(1, stages)] + [{'data': up}, {'data': down}])

    for c in w_copies(0):
        c.wait()

    def fwd_wait(i):
        lower = i < micros

        @pl.when(first & lower)
        def _():
            x_copy(i).wait()

        @pl.when(jnp.logical_not(first & lower))
        def _():
            f_hop(i, i).wait_recv()

    def fwd_unit(i, aslot):
        v = i // micros
        lower = i < micros
        upper = jnp.logical_not(lower)
        o = lax.rem(i, micros)
        slot = jnp.where(last, i + micros, i)
        final = last & upper
        a = abuf.at[aslot]

        @pl.when(lower)
        def _():
            h_keep(i).start()
            h_push(i, 0).start()
            h_push(i, 1).start()

        @pl.when(upper)
        def _():
            f_hop(o, o).wait_send()
            h_push(o, 0).wait_recv()
            h_push(o, 1).wait_recv()
            h_forward(o, 0).start()
            h_forward(o, 1).start()

        @pl.when(jnp.logical_not(final))
        def _():
            for cols in slices(hid, fb):
                a[:, cols] = gelu_only(dot(hbuf[i], wi[v, :, cols])).astype(BF16)

        for cols in slices(dim, nb):
            out = hbuf[i, :, cols].astype(F32) + dot(a[...], wo[v, :, cols])
            obuf[o, :, cols] = out.astype(BF16)

            @pl.when(jnp.logical_not(final))
            def _():
                f_hop(i, slot, cols).start()

        @pl.when(final)
        def _():
            y_copy(o).start()

    def bwd_unit(m, v, slot):
        q = qbuf.at[slot]
        upper = m < micros
        o = lax.rem(m, micros)

        @pl.when(last & upper)
        def _():
            g_copy(m).wait()
            y_copy(m).wait()

        @pl.when(jnp.logical_not(last & upper))
        def _():
            b_hop(m).wait_recv()

        @pl.when(inner & upper)
        def _():
            f_hop(micros + m, micros + m).wait_send()

        @pl.when(defer & upper & (m >= 2))
        def _():
            q_keep(m - 2).wait()

        @pl.when(jnp.logical_not(upper))
        def _():
            b_hop(o).wait_send()
            e_low_keep(o).start()

        for cols in slices(hid, fb):
            q[:, cols] = (slope[:, cols] * dot_nt(ebuf[m], wo[v, cols, :])).astype(BF16)
        for cols in slices(dim, nb):
            out = ebuf[m, :, cols].astype(F32) + dot_nt(q[...], wi[v, cols, :])
            obuf[o, :, cols] = out.astype(BF16)

            @pl.when(jnp.logical_not(first))
            def _():
                b_hop(m, cols).start()

            @pl.when(first)
            def _():
                entry(m, cols).start()
                e_push(m, 0, cols).start()
                e_push(m, 1, cols).start()

        @pl.when(first)
        def _():
            e_keep(m).start()

            @pl.when(m >= 1)
            def _():
                far(m - 1)

        @pl.when(defer & upper)
        def _():
            q_keep(m).start()

        @pl.when(jnp.logical_not(upper))
        def _():
            for c in low_keep(o):
                c.start()

    def far(m):
        for j in range(2):
            e_push(m, j).wait_recv()
        for j in range(2):
            e_forward(m, j).start()

    def weight_unit(m, k):
        for cols in slices(hid, wb):
            gin[:, cols] += dot_tn(hbuf[micros + m], qbuf[k, :, cols])
            gout[cols, :] += dot_tn(abuf[k, :, cols], ebuf[m])

    def step(t):
        m = t - micros - lag
        low = m - micros
        upper = (m >= 0) & (low < 0)
        active = (m >= 0) & (low < heads)
        v = jnp.where(low < 0, 1, 0)
        slot = jnp.where(low < 0, lax.rem(t + micros + lag, 2), 0)
        w = jnp.where(defer, low, m)

        @pl.when(t == micros)
        def _():
            gin[...] = jnp.zeros_like(gin)
            gout[...] = jnp.zeros_like(gout)
            for c in w_copies(1):
                c.wait()

        @pl.when(defer & (low == 0))
        def _():
            for n in range(micros - 2, micros):
                a_keep(n).wait()
                q_keep(n).wait()

        @pl.when(defer & (low >= 0))
        def _():
            for c in loads(low):
                c.start()

        early = last & upper

        @pl.when(early)
        def _():
            fwd_wait(t)

        @pl.when(active)
        def _():
            @pl.when(defer & upper & (m >= 2))
            def _():
                a_keep(m - 2).wait()

            @pl.when(low >= 1)
            def _():
                for c in low_keep(low - 1):
                    c.wait()

            act_pass(hbuf.at[jnp.where(low < 0, micros + m, low)], wi.at[v], abuf.at[slot], slope, fb)

            @pl.when(defer & upper)
            def _():
                a_keep(m).start()

        @pl.when(t < 2 * micros)
        def _():
            @pl.when(jnp.logical_not(early))
            def _():
                fwd_wait(t)

            fwd_unit(t, jnp.where(early, slot, 2))

        @pl.when(active)
        def _():
            bwd_unit(m, v, slot)

        @pl.when(defer & (low >= 0))
        def _():
            for c in loads(low):
                c.wait()

        @pl.when((w >= 0) & (w < micros))
        def _():
            weight_unit(w, jnp.where(defer, 1, slot))

    loop(0, 2 * micros + lag + jnp.where(defer, micros, heads), step)

    outs = (pltpu.make_async_copy(gin, gin_hbm, o_sem.at[0]), pltpu.make_async_copy(gout, gout_hbm, o_sem.at[1]))
    for c in outs:
        c.start()

    @pl.when(first)
    def _():
        far(micros - 1)

    def drain(m):
        h_keep(m).wait()
        h_push(m, 0).wait_send()
        h_push(m, 1).wait_send()
        h_forward(m, 0).wait_send()
        h_forward(m, 1).wait_send()
        h_whole(m).wait_recv()

        @pl.when(jnp.logical_not(first) & (m >= heads))
        def _():
            b_hop(m).wait_send()

        @pl.when(m < heads)
        def _():
            b_hop(micros + m).wait_send()

        @pl.when((m >= heads) & (m < arrivals))
        def _():
            b_hop(micros + m).wait_recv()
            e_low_keep(m).start()

        @pl.when(m < arrivals)
        def _():
            e_low_keep(m).wait()

        @pl.when(first)
        def _():
            entry(m).wait_send()
            e_keep(m).wait()
            for j in range(2):
                e_push(m, j).wait_send()
                e_forward(m, j).wait_send()
            e_whole(m).wait_recv()

    loop(0, micros, drain)

    @pl.when(heads > 0)
    def _():
        for c in low_keep(heads - 1):
            c.wait()

    for c in outs:
        c.wait()


def run_front(stages, levels, x, g, w_in, w_out):
    micros, tokens, dim = x.shape
    _, _, hid = w_in.shape
    chunks = 3 if dim % 384 == 0 else 1
    dma = pltpu.SemaphoreType.DMA

    def rows(n):
        return jax.ShapeDtypeStruct((n * micros, tokens, dim), BF16)

    def acts(n):
        return jax.ShapeDtypeStruct((n * micros, tokens, hid), BF16)

    return pl.pallas_call(
        functools.partial(front_kernel, stages, levels, micros, chunks),
        out_shape=(rows(4), rows(1), rows(4), jax.ShapeDtypeStruct((dim, hid), F32), jax.ShapeDtypeStruct((hid, dim), F32),
                   acts(1), acts(1), acts(levels), acts(levels), rows(levels)),
        in_specs=[ANY] * 4, out_specs=(ANY,) * 10,
        scratch_shapes=[
            pltpu.VMEM((2, dim, hid), BF16), pltpu.VMEM((2, hid, dim), BF16),
            pltpu.VMEM((2 * micros, tokens, dim), BF16), pltpu.VMEM((micros, tokens, dim), BF16), pltpu.VMEM((2 * micros, tokens, dim), BF16),
            pltpu.VMEM((dim, hid), F32), pltpu.VMEM((hid, dim), F32),
            pltpu.VMEM((3, tokens, hid), BF16), pltpu.VMEM((2, tokens, hid), BF16), pltpu.VMEM((tokens, hid), F32),
            dma((2, 2)), dma((micros,)), dma((micros,)), dma((2 * micros,)), dma((2 * micros,)), dma((2 * micros,)), dma((2 * micros,)), dma((micros,)),
            dma((micros,)), dma((4, micros)), dma((3, micros)), dma((micros,)), dma((4, micros)), dma((3, micros)),
            dma((2, micros)), dma((2,)), dma((2,)), dma((2 + micros,)),
        ],
        compiler_params=pltpu.CompilerParams(collective_id=0, has_side_effects=True, vmem_limit_bytes=VMEM_LIMIT),
        cost_estimate=pl.CostEstimate(flops=micros * 18 * tokens * dim * hid, bytes_accessed=4 * micros * tokens * hid * 2,
                                      transcendentals=3 * micros * tokens * hid),
        name='front',
    )(x, g, w_in, w_out)


def wide_kernel(stages, micros, chunks, hall, eall, _y, _a, _q, _e, wi_hbm, wo_hbm, a_out, q_out, e_out, dx_out, y_out,
                wi, wo, hbuf, obuf, ebuf, abuf, qbuf,
                w_sem, h_sem, n_send, b_send, b_recv, dx_sem, dx_send, dx_recv, y_send, y_recv, s_sem, l_sem):
    s = lax.axis_index('stage')
    nxt, prv = lax.rem(s + 1, stages), lax.rem(s + stages - 1, stages)
    dim, hid = wi.shape
    units = ebuf.shape[0]
    nb = dim // chunks
    fb = pick_block(hid, 768)
    hslots = hbuf.shape[0]
    first = s == 0
    last = s == stages - 1
    heads, arrivals = head_units(s, micros), head_arrivals(s, stages, micros)

    w_copies = (pltpu.make_async_copy(wi_hbm.at[0], wi, w_sem.at[0]), pltpu.make_async_copy(wo_hbm.at[0], wo, w_sem.at[1]))

    def h_copy(i):
        return pltpu.make_async_copy(hall.at[i], hbuf.at[lax.rem(i, hslots)], h_sem.at[lax.rem(i, hslots)])

    def entry(i):
        return pltpu.make_async_remote_copy(
            src_ref=eall.at[i], dst_ref=ebuf.at[i], send_sem=n_send.at[i], recv_sem=b_recv.at[i],
            device_id={'stage': prv}, device_id_type=MESH)

    def b_hop(i, cols=slice(None)):
        o = lax.rem(i, micros)
        return pltpu.make_async_remote_copy(
            src_ref=obuf.at[o, :, cols], dst_ref=ebuf.at[i, :, cols], send_sem=b_send.at[o], recv_sem=b_recv.at[i],
            device_id={'stage': prv}, device_id_type=MESH)

    def dx_copy(m):
        return pltpu.make_async_copy(obuf.at[m], dx_out.at[m], dx_sem.at[m])

    def dx_hop(m, src):
        return pltpu.make_async_remote_copy(
            src_ref=src.at[m], dst_ref=dx_out.at[m], send_sem=dx_send.at[m], recv_sem=dx_recv.at[m],
            device_id={'stage': nxt}, device_id_type=MESH)

    def y_hop(m):
        return pltpu.make_async_remote_copy(
            src_ref=y_out.at[m], dst_ref=y_out.at[m], send_sem=y_send.at[m], recv_sem=y_recv.at[m],
            device_id={'stage': nxt}, device_id_type=MESH)

    def e_load(i):
        return pltpu.make_async_copy(e_out.at[i], ebuf.at[i], l_sem.at[i])

    def relay(i):
        my = jnp.where(last, i, i - 2 - 2 * s)
        mx = i - 1 - 2 * s

        @pl.when((my >= 0) & (my < micros))
        def _():
            @pl.when(jnp.logical_not(last))
            def _():
                y_hop(my).wait_recv()

            @pl.when(s != stages - 2)
            def _():
                y_hop(my).start()

        @pl.when((mx >= 0) & (mx < micros) & jnp.logical_not(first))
        def _():
            dx_hop(mx, dx_out).wait_recv()

            @pl.when(jnp.logical_not(last))
            def _():
                dx_hop(mx, dx_out).start()

    def keep(i):
        k = lax.rem(i, 2)
        return (pltpu.make_async_copy(abuf.at[k], a_out.at[i], s_sem.at[0, k]), pltpu.make_async_copy(qbuf.at[k], q_out.at[i], s_sem.at[1, k]),
                pltpu.make_async_copy(ebuf.at[i], e_out.at[i], s_sem.at[2, k]))

    for c in w_copies:
        c.start()
    for i in range(hslots - 1):
        h_copy(heads + i).start()
    loop(heads, arrivals, lambda i: e_load(i).start())

    signal_all([{'stage': lax.rem(s + step, stages)} for step in range(1, stages)])

    @pl.when(first)
    def _():
        loop(micros, units, lambda i: entry(i).start())

    for c in w_copies:
        c.wait()

    def unit(i):
        k = lax.rem(i, 2)
        a, q, h = abuf.at[k], qbuf.at[k], hbuf.at[lax.rem(i, hslots)]
        o = lax.rem(i, micros)

        @pl.when(i + hslots - 1 < units)
        def _():
            h_copy(i + hslots - 1).start()

        h_copy(i).wait()

        @pl.when(i < arrivals)
        def _():
            e_load(i).wait()

        @pl.when(i >= arrivals)
        def _():
            b_hop(i).wait_recv()

        @pl.when(i >= heads + 2)
        def _():
            for c in keep(i - 2):
                c.wait()

        relay(i - heads)

        @pl.when(jnp.logical_not(first) & (i >= heads + micros))
        def _():
            b_hop(i - micros).wait_send()

        for cols in slices(hid, fb):
            act, der = gelu_and_slope(dot(h[...], wi[:, cols]))
            a[:, cols] = act.astype(BF16)
            q[:, cols] = (der * dot_nt(ebuf[i], wo[cols, :])).astype(BF16)

        @pl.when(jnp.logical_not(first) | (i < micros))
        def _():
            for cols in slices(dim, nb):
                out = ebuf[i, :, cols].astype(F32) + dot_nt(q[...], wi[cols, :])
                obuf[o, :, cols] = out.astype(BF16)

                @pl.when(jnp.logical_not(first))
                def _():
                    b_hop(i, cols).start()

        @pl.when(first & (i < micros))
        def _():
            dx_copy(i).start()
            dx_hop(i, obuf).start()

        for c in keep(i):
            c.start()

    loop(heads, units, unit)
    loop(units - heads, jnp.maximum(units - heads, micros + 2 * stages - 1), relay)

    @pl.when(first)
    def _():
        loop(micros, units, lambda i: entry(i).wait_send())
        loop(0, micros, lambda m: dx_copy(m).wait())

    @pl.when(jnp.logical_not(first))
    def _():
        loop(units - micros, units, lambda i: b_hop(i).wait_send())

    @pl.when(jnp.logical_not(last))
    def _():
        loop(0, micros, lambda m: dx_hop(m, dx_out).wait_send())

    @pl.when(s != stages - 2)
    def _():
        loop(0, micros, lambda m: y_hop(m).wait_send())

    for i in (units - 2, units - 1):
        for c in keep(i):
            c.wait()


def run_wide(stages, micros, hall, eall, y, alow, qlow, elow, w_in, w_out):
    units, tokens, dim = hall.shape
    _, _, hid = w_in.shape
    chunks = 3 if dim % 384 == 0 else 1
    dma = pltpu.SemaphoreType.DMA
    small = jax.ShapeDtypeStruct((micros, tokens, dim), BF16)
    acts = jax.ShapeDtypeStruct((units, tokens, hid), BF16)
    return pl.pallas_call(
        functools.partial(wide_kernel, stages, micros, chunks),
        out_shape=(acts, acts, jax.ShapeDtypeStruct((units, tokens, dim), BF16), small, small),
        in_specs=[ANY] * 8, out_specs=(ANY,) * 5,
        scratch_shapes=[
            pltpu.VMEM((dim, hid), BF16), pltpu.VMEM((hid, dim), BF16),
            pltpu.VMEM((4, tokens, dim), BF16), pltpu.VMEM((micros, tokens, dim), BF16), pltpu.VMEM((units, tokens, dim), BF16),
            pltpu.VMEM((2, tokens, hid), BF16), pltpu.VMEM((2, tokens, hid), BF16),
            dma((2,)), dma((4,)), dma((units,)), dma((micros,)), dma((units,)), dma((micros,)), dma((micros,)), dma((micros,)),
            dma((micros,)), dma((micros,)), dma((3, 2)), dma((micros,)),
        ],
        input_output_aliases={2: 4, 3: 0, 4: 1, 5: 2},
        compiler_params=pltpu.CompilerParams(collective_id=1, has_side_effects=True, vmem_limit_bytes=VMEM_LIMIT),
        cost_estimate=pl.CostEstimate(flops=units * 6 * tokens * dim * hid, bytes_accessed=units * tokens * hid * 4,
                                      transcendentals=units * tokens * hid),
        name='wide',
    )(hall, eall, y, alow, qlow, elow, w_in, w_out)


def wgrad_kernel(lhs, rhs, out):
    @pl.when(pl.program_id(1) == 0)
    def _():
        out[...] = jnp.zeros_like(out)

    out[0] += dot_tn(lhs[...], rhs[...])


def run_wgrad(lhs, rhs, split_lhs, name):
    lhs, rhs = lhs.reshape(-1, lhs.shape[-1]), rhs.reshape(-1, rhs.shape[-1])
    tokens, m, n = lhs.shape[0], lhs.shape[1], rhs.shape[1]
    kb = pick_block(tokens, 2048)
    fb = pick_block(m if split_lhs else n, 1024)
    if split_lhs:
        grid, block = (m // fb, tokens // kb), (1, fb, n)
        lhs_spec, rhs_spec = pl.BlockSpec((kb, fb), lambda j, k: (k, j)), pl.BlockSpec((kb, n), lambda j, k: (k, 0))
        place = lambda j, k: (0, j, 0)
    else:
        grid, block = (n // fb, tokens // kb), (1, m, fb)
        lhs_spec, rhs_spec = pl.BlockSpec((kb, m), lambda j, k: (k, 0)), pl.BlockSpec((kb, fb), lambda j, k: (k, j))
        place = lambda j, k: (0, 0, j)
    return pl.pallas_call(
        wgrad_kernel, grid=grid, out_shape=jax.ShapeDtypeStruct((2, m, n), F32), in_specs=[lhs_spec, rhs_spec],
        out_specs=pl.BlockSpec(block, place), compiler_params=pltpu.CompilerParams(vmem_limit_bytes=VMEM_LIMIT),
        cost_estimate=pl.CostEstimate(flops=2 * tokens * m * n, bytes_accessed=2 * tokens * (m + n) + 4 * m * n, transcendentals=0),
        name=name,
    )(lhs, rhs)


def place_kernel(dx, y, dx_out, y_out):
    dx_out[...] = dx[...]
    y_out[...] = y[...]


def run_place(dx, y):
    spec = pl.BlockSpec((1,) + dx.shape[1:], lambda i: (i, 0, 0))
    shape = jax.ShapeDtypeStruct(dx.shape, BF16)
    return pl.pallas_call(
        place_kernel, grid=(dx.shape[0],), out_shape=(shape, shape), in_specs=[spec] * 2, out_specs=(spec, spec),
        cost_estimate=pl.CostEstimate(flops=dx.size, bytes_accessed=8 * dx.size, transcendentals=0), name='place',
    )(dx, y)


def solution(mesh):
    stages, levels = mesh.shape['stage'], mesh.shape['data']

    def local_fn(x, g, w_in, w_out):
        wi, wo = w_in[:, 0], w_out[:, 0]
        hall, y, eall, gin_up, gout_up, _, _, alow, qlow, elow = run_front(stages, levels, x, g, wi, wo)
        gin_up, gout_up = lax.psum((gin_up, gout_up), 'data')
        alow, qlow, elow, dx, y = run_wide(stages, x.shape[0], hall, eall, y, alow, qlow, elow, wi, wo)
        grad_in = run_wgrad(hall, qlow, False, 'gin_low')
        grad_out = run_wgrad(alow, elow, True, 'gout_low')
        dx, y = run_place(dx, y)
        grad_in = lax.dynamic_update_slice(grad_in, gin_up[None], (1, 0, 0))
        grad_out = lax.dynamic_update_slice(grad_out, gout_up[None], (1, 0, 0))
        return y, dx, grad_in[:, None], grad_out[:, None]

    spec_rows = P(('part', 'data'))
    spec_weights = P(None, 'stage')
    spec_grads = P('part', 'stage')
    return jax.shard_map(local_fn, mesh=mesh, in_specs=(spec_rows, spec_rows, spec_weights, spec_weights), out_specs=(spec_rows, spec_rows, spec_grads, spec_grads), check_vma=False)
```

```python
import functools
import jax
import jax.numpy as jnp
from jax import lax
from jax.experimental import pallas as pl
from jax.experimental.pallas import tpu as pltpu
from jax.sharding import PartitionSpec as P

MESH = pl.DeviceIdType.MESH
F32 = jnp.float32
BF16 = jnp.bfloat16
ANY = pl.BlockSpec(memory_space=pl.ANY)
GELU_A = 0.7978845608028654
GELU_B = 0.044715
VMEM_LIMIT = 67_043_328


def dot(a, b):
    return jnp.dot(a, b, preferred_element_type=F32)


def dot_nt(a, b):
    return lax.dot_general(a, b, (((1,), (1,)), ((), ())), preferred_element_type=F32)


def dot_tn(a, b):
    return lax.dot_general(a, b, (((0,), (0,)), ((), ())), preferred_element_type=F32)


def gelu_only(z):
    t = jnp.tanh(z * (GELU_A + (GELU_A * GELU_B) * (z * z)))
    return z * (0.5 * t + 0.5)


def gelu_and_slope(z):
    s = (GELU_A * GELU_B) * (z * z)
    cdf = 0.5 * jnp.tanh(z * (GELU_A + s)) + 0.5
    a = z * cdf
    return a, cdf + (a * (1.0 - cdf)) * (2.0 * GELU_A + 6.0 * s)


def pick_block(size, target):
    block = min(size, target)
    while size % block:
        block //= 2
    return block


def loop(lo, hi, fn):
    def body(i, _):
        fn(i)
        return 0
    lax.fori_loop(lo, hi, body, 0)


def head_units(s, micros):
    return jnp.minimum(jnp.maximum(s - 1, 0), micros // 2)


def head_arrivals(s, stages, micros):
    return jnp.where(s == stages - 1, micros, head_units(s + 1, micros))


def signal_all(targets):
    sem = pltpu.get_barrier_semaphore()
    for target in targets:
        pl.semaphore_signal(sem, inc=1, device_id=target, device_id_type=MESH)
    pl.semaphore_wait(sem, len(targets))


def slices(size, block):
    return [slice(b * block, (b + 1) * block) for b in range(size // block)]


def act_pass(h, wi, a, slope, fb):
    for cols in slices(wi.shape[1], fb):
        act, der = gelu_and_slope(dot(h[...], wi[:, cols]))
        a[:, cols] = act.astype(BF16)
        slope[:, cols] = der


def front_kernel(stages, levels, micros, chunks, x_hbm, g_hbm, wi_hbm, wo_hbm, hall, y_out, eall, gin_hbm, gout_hbm, aup, qup, aqlow, elow,
                 wi, wo, hbuf, obuf, ebuf, gin, gout, abuf, qbuf, slope,
                 w_sem, x_sem, g_sem, f_send, f_recv, b_send, b_recv, y_sem, h_save, h_send, h_recv, e_save, e_send, e_recv,
                 a_save, a_load, o_sem, l_save):
    s = lax.axis_index('stage')
    d = lax.axis_index('data')
    nxt, prv = lax.rem(s + 1, stages), lax.rem(s + stages - 1, stages)
    up, down = lax.rem(d + 1, levels), lax.rem(d + levels - 1, levels)
    _, dim, hid = wi.shape
    tokens = hbuf.shape[1]
    half = tokens // 2
    nb = dim // chunks
    fb = pick_block(hid, 768)
    wb = pick_block(hid, 512)
    first = s == 0
    last = s == stages - 1
    inner = jnp.logical_not(last)
    lag = jnp.minimum(3 * (stages - 1 - s), micros)
    defer = s >= stages - 2
    heads, arrivals = head_units(s, micros), head_arrivals(s, stages, micros)

    def w_copies(v):
        return (pltpu.make_async_copy(wi_hbm.at[v], wi.at[v], w_sem.at[v, 0]),
                pltpu.make_async_copy(wo_hbm.at[v], wo.at[v], w_sem.at[v, 1]))

    def x_copy(m):
        return pltpu.make_async_copy(x_hbm.at[m], hbuf.at[m], x_sem.at[m])

    def g_copy(m):
        return pltpu.make_async_copy(g_hbm.at[m], ebuf.at[m], g_sem.at[m])

    def f_hop(i, slot, cols=slice(None)):
        return pltpu.make_async_remote_copy(
            src_ref=obuf.at[lax.rem(i, micros), :, cols], dst_ref=hbuf.at[slot, :, cols], send_sem=f_send.at[i], recv_sem=f_recv.at[slot],
            device_id={'stage': nxt}, device_id_type=MESH)

    def b_hop(m, cols=slice(None)):
        return pltpu.make_async_remote_copy(
            src_ref=obuf.at[lax.rem(m, micros), :, cols], dst_ref=ebuf.at[m, :, cols], send_sem=b_send.at[m], recv_sem=b_recv.at[m],
            device_id={'stage': prv}, device_id_type=MESH)

    def entry(m, cols=slice(None)):
        return pltpu.make_async_remote_copy(
            src_ref=obuf.at[m, :, cols], dst_ref=ebuf.at[micros + m, :, cols], send_sem=b_send.at[m], recv_sem=b_recv.at[micros + m],
            device_id={'stage': prv}, device_id_type=MESH)

    def low_keep(k):
        return (pltpu.make_async_copy(abuf.at[0], aqlow.at[k, 0], l_save.at[0]), pltpu.make_async_copy(qbuf.at[0], aqlow.at[k, 1], l_save.at[1]))

    def e_low_keep(k):
        return pltpu.make_async_copy(ebuf.at[micros + k], elow.at[k], l_save.at[2 + k])

    def y_copy(m):
        return pltpu.make_async_copy(obuf.at[m], y_out.at[m], y_sem.at[m])

    def h_keep(m):
        return pltpu.make_async_copy(hbuf.at[m], hall.at[m], h_save.at[m])

    def h_push(m, j):
        return pltpu.make_async_remote_copy(
            src_ref=hbuf.at[m], dst_ref=hall.at[(2 - j) * micros + m], send_sem=h_send.at[j, m], recv_sem=h_recv.at[1 - j, m],
            device_id={'data': (up, down)[j]}, device_id_type=MESH)

    def h_forward(m, j):
        rows = (slice(0, half), slice(half, tokens))[j]
        return pltpu.make_async_remote_copy(
            src_ref=hall.at[(2 - j) * micros + m, rows], dst_ref=hall.at[3 * micros + m, rows], send_sem=h_send.at[2 + j, m],
            recv_sem=h_recv.at[2, m], device_id={'data': (up, down)[j]}, device_id_type=MESH)

    def h_whole(m):
        return pltpu.make_async_remote_copy(
            src_ref=hall.at[m], dst_ref=hall.at[3 * micros + m], send_sem=h_send.at[2, m], recv_sem=h_recv.at[2, m],
            device_id={'data': up}, device_id_type=MESH)

    def e_keep(m):
        return pltpu.make_async_copy(obuf.at[m], eall.at[m], e_save.at[m])

    def e_push(m, j, cols=slice(None)):
        return pltpu.make_async_remote_copy(
            src_ref=obuf.at[m, :, cols], dst_ref=eall.at[(2 - j) * micros + m, :, cols], send_sem=e_send.at[j, m], recv_sem=e_recv.at[1 - j, m],
            device_id={'data': (up, down)[j]}, device_id_type=MESH)

    def e_forward(m, j):
        rows = (slice(0, half), slice(half, tokens))[j]
        return pltpu.make_async_remote_copy(
            src_ref=eall.at[(2 - j) * micros + m, rows], dst_ref=eall.at[3 * micros + m, rows], send_sem=e_send.at[2 + j, m],
            recv_sem=e_recv.at[2, m], device_id={'data': (up, down)[j]}, device_id_type=MESH)

    def e_direct(m):
        return pltpu.make_async_remote_copy(
            src_ref=obuf.at[m], dst_ref=eall.at[3 * micros + m], send_sem=e_send.at[2, m], recv_sem=e_recv.at[2, m],
            device_id={'data': lax.rem(d + 2, levels)}, device_id_type=MESH)

    def e_whole(m):
        return pltpu.make_async_remote_copy(
            src_ref=eall.at[m], dst_ref=eall.at[3 * micros + m], send_sem=e_send.at[2, m], recv_sem=e_recv.at[2, m],
            device_id={'data': up}, device_id_type=MESH)

    def a_keep(m):
        return pltpu.make_async_copy(abuf.at[lax.rem(m, 2)], aup.at[m], a_save.at[0, m])

    def q_keep(m):
        return pltpu.make_async_copy(qbuf.at[lax.rem(m, 2)], qup.at[m], a_save.at[1, m])

    def loads(m):
        return (pltpu.make_async_copy(aup.at[m], abuf.at[1], a_load.at[0]), pltpu.make_async_copy(qup.at[m], qbuf.at[1], a_load.at[1]))

    for v in range(2):
        for c in w_copies(v):
            c.start()

    @pl.when(first)
    def _():
        loop(0, micros, lambda m: x_copy(m).start())

    @pl.when(last)
    def _():
        loop(0, micros, lambda m: g_copy(m).start())

    signal_all([{'stage': lax.rem(s + step, stages)} for step in range(1, stages)] + [{'data': up}, {'data': down}, {'data': lax.rem(d + 2, levels)}])

    for c in w_copies(0):
        c.wait()

    def fwd_wait(i):
        lower = i < micros

        @pl.when(first & lower)
        def _():
            x_copy(i).wait()

        @pl.when(jnp.logical_not(first & lower))
        def _():
            f_hop(i, i).wait_recv()

    def fwd_unit(i, aslot):
        v = i // micros
        lower = i < micros
        upper = jnp.logical_not(lower)
        o = lax.rem(i, micros)
        slot = jnp.where(last, i + micros, i)
        final = last & upper
        a = abuf.at[aslot]

        @pl.when(lower)
        def _():
            h_keep(i).start()
            h_push(i, 0).start()
            h_push(i, 1).start()

        @pl.when(upper)
        def _():
            f_hop(o, o).wait_send()
            h_push(o, 0).wait_recv()
            h_push(o, 1).wait_recv()
            h_forward(o, 0).start()
            h_forward(o, 1).start()

        @pl.when(jnp.logical_not(final))
        def _():
            for cols in slices(hid, fb):
                a[:, cols] = gelu_only(dot(hbuf[i], wi[v, :, cols])).astype(BF16)

        for cols in slices(dim, nb):
            out = hbuf[i, :, cols].astype(F32) + dot(a[...], wo[v, :, cols])
            obuf[o, :, cols] = out.astype(BF16)

            @pl.when(jnp.logical_not(final))
            def _():
                f_hop(i, slot, cols).start()

        @pl.when(final)
        def _():
            y_copy(o).start()

    def bwd_unit(m, v, slot):
        q = qbuf.at[slot]
        upper = m < micros
        o = lax.rem(m, micros)

        @pl.when(last & upper)
        def _():
            g_copy(m).wait()
            y_copy(m).wait()

        @pl.when(jnp.logical_not(last & upper))
        def _():
            b_hop(m).wait_recv()

        @pl.when(inner & upper)
        def _():
            f_hop(micros + m, micros + m).wait_send()

        @pl.when(defer & upper & (m >= 2))
        def _():
            q_keep(m - 2).wait()

        @pl.when(jnp.logical_not(upper))
        def _():
            b_hop(o).wait_send()
            e_low_keep(o).start()

        for cols in slices(hid, fb):
            q[:, cols] = (slope[:, cols] * dot_nt(ebuf[m], wo[v, cols, :])).astype(BF16)
        for cols in slices(dim, nb):
            out = ebuf[m, :, cols].astype(F32) + dot_nt(q[...], wi[v, cols, :])
            obuf[o, :, cols] = out.astype(BF16)

            @pl.when(jnp.logical_not(first))
            def _():
                b_hop(m, cols).start()

            @pl.when(first)
            def _():
                entry(m, cols).start()
                e_push(m, 0, cols).start()
                e_push(m, 1, cols).start()

        @pl.when(first)
        def _():
            e_keep(m).start()

            @pl.when(m >= 1)
            def _():
                far(m - 1)

            @pl.when(m == micros - 1)
            def _():
                e_direct(m).start()

        @pl.when(defer & upper)
        def _():
            q_keep(m).start()

        @pl.when(jnp.logical_not(upper))
        def _():
            for c in low_keep(o):
                c.start()

    def far(m):
        for j in range(2):
            e_push(m, j).wait_recv()
        for j in range(2):
            e_forward(m, j).start()

    def weight_unit(m, k):
        for cols in slices(hid, wb):
            gin[:, cols] += dot_tn(hbuf[micros + m], qbuf[k, :, cols])
            gout[cols, :] += dot_tn(abuf[k, :, cols], ebuf[m])

    def step(t):
        m = t - micros - lag
        low = m - micros
        upper = (m >= 0) & (low < 0)
        active = (m >= 0) & (low < heads)
        v = jnp.where(low < 0, 1, 0)
        slot = jnp.where(low < 0, lax.rem(t + micros + lag, 2), 0)
        w = jnp.where(defer, low, m)

        @pl.when(t == micros)
        def _():
            gin[...] = jnp.zeros_like(gin)
            gout[...] = jnp.zeros_like(gout)
            for c in w_copies(1):
                c.wait()

        @pl.when(defer & (low == 0))
        def _():
            for n in range(micros - 2, micros):
                a_keep(n).wait()
                q_keep(n).wait()

        @pl.when(defer & (low >= 0))
        def _():
            for c in loads(low):
                c.start()

        early = last & upper

        @pl.when(early)
        def _():
            fwd_wait(t)

        @pl.when(active)
        def _():
            @pl.when(defer & upper & (m >= 2))
            def _():
                a_keep(m - 2).wait()

            @pl.when(low >= 1)
            def _():
                for c in low_keep(low - 1):
                    c.wait()

            act_pass(hbuf.at[jnp.where(low < 0, micros + m, low)], wi.at[v], abuf.at[slot], slope, fb)

            @pl.when(defer & upper)
            def _():
                a_keep(m).start()

        @pl.when(t < 2 * micros)
        def _():
            @pl.when(jnp.logical_not(early))
            def _():
                fwd_wait(t)

            fwd_unit(t, jnp.where(early, slot, 2))

        @pl.when(active)
        def _():
            bwd_unit(m, v, slot)

        @pl.when(defer & (low >= 0))
        def _():
            for c in loads(low):
                c.wait()

        @pl.when((w >= 0) & (w < micros))
        def _():
            weight_unit(w, jnp.where(defer, 1, slot))

    loop(0, 2 * micros + lag + jnp.where(defer, micros, heads), step)

    outs = (pltpu.make_async_copy(gin, gin_hbm, o_sem.at[0]), pltpu.make_async_copy(gout, gout_hbm, o_sem.at[1]))
    for c in outs:
        c.start()

    def drain(m):
        h_keep(m).wait()
        h_push(m, 0).wait_send()
        h_push(m, 1).wait_send()
        h_forward(m, 0).wait_send()
        h_forward(m, 1).wait_send()
        h_whole(m).wait_recv()

        @pl.when(jnp.logical_not(first) & (m >= heads))
        def _():
            b_hop(m).wait_send()

        @pl.when(m < heads)
        def _():
            b_hop(micros + m).wait_send()

        @pl.when((m >= heads) & (m < arrivals))
        def _():
            b_hop(micros + m).wait_recv()
            e_low_keep(m).start()

        @pl.when(m < arrivals)
        def _():
            e_low_keep(m).wait()

        @pl.when(first)
        def _():
            entry(m).wait_send()
            e_keep(m).wait()
            for j in range(2):
                e_push(m, j).wait_send()
            e_whole(m).wait_recv()

            @pl.when(m < micros - 1)
            def _():
                for j in range(2):
                    e_forward(m, j).wait_send()

            @pl.when(m == micros - 1)
            def _():
                e_direct(m).wait_send()
                for j in range(2):
                    e_push(m, j).wait_recv()

    loop(0, micros, drain)

    @pl.when(heads > 0)
    def _():
        for c in low_keep(heads - 1):
            c.wait()

    for c in outs:
        c.wait()


def run_front(stages, levels, x, g, w_in, w_out):
    micros, tokens, dim = x.shape
    _, _, hid = w_in.shape
    chunks = 3 if dim % 384 == 0 else 1
    dma = pltpu.SemaphoreType.DMA

    def rows(n):
        return jax.ShapeDtypeStruct((n * micros, tokens, dim), BF16)

    def acts(n):
        return jax.ShapeDtypeStruct((n * micros, tokens, hid), BF16)

    return pl.pallas_call(
        functools.partial(front_kernel, stages, levels, micros, chunks),
        out_shape=(rows(4), rows(1), rows(4), jax.ShapeDtypeStruct((dim, hid), F32), jax.ShapeDtypeStruct((hid, dim), F32),
                   acts(1), acts(1), jax.ShapeDtypeStruct((levels * micros, 2, tokens, hid), BF16), rows(levels)),
        in_specs=[ANY] * 4, out_specs=(ANY,) * 9,
        scratch_shapes=[
            pltpu.VMEM((2, dim, hid), BF16), pltpu.VMEM((2, hid, dim), BF16),
            pltpu.VMEM((2 * micros, tokens, dim), BF16), pltpu.VMEM((micros, tokens, dim), BF16), pltpu.VMEM((2 * micros, tokens, dim), BF16),
            pltpu.VMEM((dim, hid), F32), pltpu.VMEM((hid, dim), F32),
            pltpu.VMEM((3, tokens, hid), BF16), pltpu.VMEM((2, tokens, hid), BF16), pltpu.VMEM((tokens, hid), F32),
            dma((2, 2)), dma((micros,)), dma((micros,)), dma((2 * micros,)), dma((2 * micros,)), dma((2 * micros,)), dma((2 * micros,)), dma((micros,)),
            dma((micros,)), dma((4, micros)), dma((3, micros)), dma((micros,)), dma((4, micros)), dma((3, micros)),
            dma((2, micros)), dma((2,)), dma((2,)), dma((2 + micros,)),
        ],
        compiler_params=pltpu.CompilerParams(collective_id=0, has_side_effects=True, vmem_limit_bytes=VMEM_LIMIT),
        cost_estimate=pl.CostEstimate(flops=micros * 18 * tokens * dim * hid, bytes_accessed=4 * micros * tokens * hid * 2,
                                      transcendentals=3 * micros * tokens * hid),
        name='front',
    )(x, g, w_in, w_out)


def wide_kernel(stages, micros, hall, eall, _y, _aq, _e, wi_hbm, wo_hbm, aq_out, e_out, dx_out, y_out,
                wi, wo, hbuf, obuf, ebuf, aqbuf,
                w_sem, h_sem, n_send, b_send, b_recv, dx_sem, dx_send, dx_recv, y_send, y_recv, s_sem, k_sem, l_sem):
    s = lax.axis_index('stage')
    nxt, prv = lax.rem(s + 1, stages), lax.rem(s + stages - 1, stages)
    dim, hid = wi.shape
    units = ebuf.shape[0]
    fb = pick_block(hid, 768)
    ob = pick_block(dim, 256)
    groups = units // micros
    first = s == 0
    last = s == stages - 1
    heads, arrivals = head_units(s, micros), head_arrivals(s, stages, micros)

    w_copies = (pltpu.make_async_copy(wi_hbm.at[0], wi, w_sem.at[0]), pltpu.make_async_copy(wo_hbm.at[0], wo, w_sem.at[1]))

    def part(k):
        return pl.ds(k * micros, micros)

    def h_copy(k):
        return pltpu.make_async_copy(hall.at[part(k)], hbuf.at[part(k)], h_sem.at[k])

    def e_part(k):
        return pltpu.make_async_copy(ebuf.at[part(k)], e_out.at[part(k)], k_sem.at[k])

    def e_keep(i):
        return pltpu.make_async_copy(ebuf.at[i], e_out.at[i], l_sem.at[i])

    def entry(i):
        return pltpu.make_async_remote_copy(
            src_ref=eall.at[i], dst_ref=ebuf.at[i], send_sem=n_send.at[i], recv_sem=b_recv.at[i],
            device_id={'stage': prv}, device_id_type=MESH)

    def b_hop(i):
        o = lax.rem(i, micros)
        return pltpu.make_async_remote_copy(
            src_ref=obuf.at[o], dst_ref=ebuf.at[i], send_sem=b_send.at[o], recv_sem=b_recv.at[i],
            device_id={'stage': prv}, device_id_type=MESH)

    def dx_copy(m):
        return pltpu.make_async_copy(obuf.at[m], dx_out.at[m], dx_sem.at[m])

    def dx_hop(m, src):
        return pltpu.make_async_remote_copy(
            src_ref=src.at[m], dst_ref=dx_out.at[m], send_sem=dx_send.at[m], recv_sem=dx_recv.at[m],
            device_id={'stage': nxt}, device_id_type=MESH)

    def y_hop(m):
        return pltpu.make_async_remote_copy(
            src_ref=y_out.at[m], dst_ref=y_out.at[m], send_sem=y_send.at[m], recv_sem=y_recv.at[m],
            device_id={'stage': nxt}, device_id_type=MESH)

    def e_load(i):
        return pltpu.make_async_copy(e_out.at[i], ebuf.at[i], l_sem.at[i])

    def relay(i):
        my = jnp.where(last, i, i - 2 - 2 * s)
        mx = i - 1 - 2 * s

        @pl.when((my >= 0) & (my < micros))
        def _():
            @pl.when(jnp.logical_not(last))
            def _():
                y_hop(my).wait_recv()

            @pl.when(s != stages - 2)
            def _():
                y_hop(my).start()

        @pl.when((mx >= 0) & (mx < micros) & jnp.logical_not(first))
        def _():
            dx_hop(mx, dx_out).wait_recv()

            @pl.when(jnp.logical_not(last))
            def _():
                dx_hop(mx, dx_out).start()

    def keep(i):
        k = lax.rem(i, 2)
        return pltpu.make_async_copy(aqbuf.at[k], aq_out.at[i], s_sem.at[k])

    for c in w_copies:
        c.start()
    for k in range(groups):
        h_copy(k).start()
    loop(heads, arrivals, lambda i: e_load(i).start())

    signal_all([{'stage': lax.rem(s + step, stages)} for step in range(1, stages)])

    @pl.when(first)
    def _():
        loop(micros, units, lambda i: entry(i).start())

    for c in w_copies:
        c.wait()

    def unit(i):
        k = lax.rem(i, 2)
        a, q = aqbuf.at[k, 0], aqbuf.at[k, 1]
        o = lax.rem(i, micros)

        @pl.when((o == 0) | (i == heads))
        def _():
            h_copy(i // micros).wait()

        @pl.when(i < arrivals)
        def _():
            e_load(i).wait()

        @pl.when(i >= arrivals)
        def _():
            b_hop(i).wait_recv()

        @pl.when(i >= heads + 2)
        def _():
            keep(i - 2).wait()

        relay(i - heads)

        for cols in slices(hid, fb):
            act, der = gelu_and_slope(dot(hbuf[i], wi[:, cols]))
            a[:, cols] = act.astype(BF16)
            q[:, cols] = (der * dot_nt(ebuf[i], wo[cols, :])).astype(BF16)

        keep(i).start()

        @pl.when(jnp.logical_not(first) & (i >= heads + micros))
        def _():
            b_hop(i - micros).wait_send()

        @pl.when(jnp.logical_not(first) | (i < micros))
        def _():
            for cols in slices(dim, ob):
                out = ebuf[i, :, cols].astype(F32) + dot_nt(q[...], wi[cols, :])
                obuf[o, :, cols] = out.astype(BF16)

            @pl.when(jnp.logical_not(first))
            def _():
                b_hop(i).start()

        @pl.when(first & (i < micros))
        def _():
            dx_copy(i).start()
            dx_hop(i, obuf).start()

        @pl.when((i >= arrivals) & (i < micros))
        def _():
            e_keep(i).start()

        @pl.when((o == micros - 1) & (i >= micros))
        def _():
            e_part(i // micros).start()

    loop(heads, units, unit)
    loop(units - heads, jnp.maximum(units - heads, micros + 2 * stages - 1), relay)

    @pl.when(first)
    def _():
        loop(micros, units, lambda i: entry(i).wait_send())
        loop(0, micros, lambda m: dx_copy(m).wait())

    @pl.when(jnp.logical_not(first))
    def _():
        loop(units - micros, units, lambda i: b_hop(i).wait_send())

    @pl.when(jnp.logical_not(last))
    def _():
        loop(0, micros, lambda m: dx_hop(m, dx_out).wait_send())

    @pl.when(s != stages - 2)
    def _():
        loop(0, micros, lambda m: y_hop(m).wait_send())

    for i in (units - 2, units - 1):
        keep(i).wait()
    loop(arrivals, micros, lambda i: e_keep(i).wait())
    for k in range(1, groups):
        e_part(k).wait()


def run_wide(stages, micros, hall, eall, y, aqlow, elow, w_in, w_out):
    units, tokens, dim = hall.shape
    _, _, hid = w_in.shape
    groups = units // micros
    dma = pltpu.SemaphoreType.DMA
    small = jax.ShapeDtypeStruct((micros, tokens, dim), BF16)
    acts = jax.ShapeDtypeStruct((units, 2, tokens, hid), BF16)
    return pl.pallas_call(
        functools.partial(wide_kernel, stages, micros),
        out_shape=(acts, jax.ShapeDtypeStruct((units, tokens, dim), BF16), small, small),
        in_specs=[ANY] * 7, out_specs=(ANY,) * 4,
        scratch_shapes=[
            pltpu.VMEM((dim, hid), BF16), pltpu.VMEM((hid, dim), BF16),
            pltpu.VMEM((units, tokens, dim), BF16), pltpu.VMEM((micros, tokens, dim), BF16), pltpu.VMEM((units, tokens, dim), BF16),
            pltpu.VMEM((2, 2, tokens, hid), BF16),
            dma((2,)), dma((groups,)), dma((units,)), dma((micros,)), dma((units,)), dma((micros,)), dma((micros,)), dma((micros,)),
            dma((micros,)), dma((micros,)), dma((2,)), dma((groups,)), dma((micros,)),
        ],
        input_output_aliases={2: 3, 3: 0, 4: 1},
        compiler_params=pltpu.CompilerParams(collective_id=1, has_side_effects=True, vmem_limit_bytes=VMEM_LIMIT),
        cost_estimate=pl.CostEstimate(flops=units * 6 * tokens * dim * hid, bytes_accessed=units * tokens * hid * 4,
                                      transcendentals=units * tokens * hid),
        name='wide',
    )(hall, eall, y, aqlow, elow, w_in, w_out)


def wgrad_kernel(lhs, rhs, *refs):
    others = (len(refs) - 1) // 2
    out = refs[others]

    @pl.when(pl.program_id(1) == 0)
    def _():
        out[...] = jnp.zeros_like(out)

    for src, dst in zip(refs[:others], refs[others + 1:]):
        dst[...] = src[...]
    lhs, rhs = (ref[...].reshape(-1, ref.shape[-1]) for ref in (lhs, rhs))
    out[0] += dot_tn(lhs, rhs)


def run_wgrad(rows, aq, which, split_lhs, others, name):
    units, tokens, dim = rows.shape
    hid = aq.shape[-1]
    ub = pick_block(units, max(1, 2048 // tokens))
    fb = pick_block(hid, 1024)
    grid = (hid // fb, units // ub)
    rows_spec = pl.BlockSpec((ub, tokens, dim), lambda j, k: (k, 0, 0))
    aq_spec = pl.BlockSpec((ub, None, tokens, fb), lambda j, k: (k, which, 0, j))
    if split_lhs:
        operands, specs = [aq, rows], [aq_spec, rows_spec]
        shape, out_spec = (2, hid, dim), pl.BlockSpec((1, fb, dim), lambda j, k: (0, j, 0))
    else:
        operands, specs = [rows, aq], [rows_spec, aq_spec]
        shape, out_spec = (2, dim, hid), pl.BlockSpec((1, dim, fb), lambda j, k: (0, 0, j))
    out_shapes, out_specs = [jax.ShapeDtypeStruct(shape, F32)], [out_spec]
    for other in others:
        count = pick_block(other.shape[0], grid[0] * grid[1])
        spec = pl.BlockSpec((other.shape[0] // count,) + other.shape[1:],
                            lambda j, k, count=count: (jnp.minimum(j * grid[1] + k, count - 1), 0, 0))
        operands.append(other)
        specs.append(spec)
        out_shapes.append(jax.ShapeDtypeStruct(other.shape, other.dtype))
        out_specs.append(spec)
    return pl.pallas_call(
        wgrad_kernel, grid=grid, out_shape=tuple(out_shapes), in_specs=specs, out_specs=tuple(out_specs),
        compiler_params=pltpu.CompilerParams(vmem_limit_bytes=VMEM_LIMIT),
        cost_estimate=pl.CostEstimate(flops=2 * units * tokens * dim * hid, bytes_accessed=2 * units * tokens * (dim + hid) + 4 * dim * hid,
                                      transcendentals=0),
        name=name,
    )(*operands)


def solution(mesh):
    stages, levels = mesh.shape['stage'], mesh.shape['data']

    def local_fn(x, g, w_in, w_out):
        wi, wo = w_in[:, 0], w_out[:, 0]
        hall, y, eall, gin_up, gout_up, _, _, aqlow, elow = run_front(stages, levels, x, g, wi, wo)
        gin_up, gout_up = lax.psum((gin_up, gout_up), 'data')
        aqlow, elow, dx, y = run_wide(stages, x.shape[0], hall, eall, y, aqlow, elow, wi, wo)
        grad_in, dx, y = run_wgrad(hall, aqlow, 1, False, (dx, y), 'gin_low')
        grad_out, = run_wgrad(elow, aqlow, 0, True, (), 'gout_low')
        grad_in = lax.dynamic_update_slice(grad_in, gin_up[None], (1, 0, 0))
        grad_out = lax.dynamic_update_slice(grad_out, gout_up[None], (1, 0, 0))
        return y, dx, grad_in[:, None], grad_out[:, None]

    spec_rows = P(('part', 'data'))
    spec_weights = P(None, 'stage')
    spec_grads = P('part', 'stage')
    return jax.shard_map(local_fn, mesh=mesh, in_specs=(spec_rows, spec_rows, spec_weights, spec_weights), out_specs=(spec_rows, spec_rows, spec_grads, spec_grads), check_vma=False)
```

```python
import functools
import jax
import jax.numpy as jnp
from jax import lax
from jax.experimental import pallas as pl
from jax.experimental.pallas import tpu as pltpu
from jax.sharding import PartitionSpec as P

MESH = pl.DeviceIdType.MESH
F32 = jnp.float32
BF16 = jnp.bfloat16
ANY = pl.BlockSpec(memory_space=pl.ANY)
GELU_A = 0.7978845608028654
GELU_B = 0.044715
VMEM_LIMIT = 67_043_328


def dot(a, b):
    return jnp.dot(a, b, preferred_element_type=F32)


def dot_nt(a, b):
    return lax.dot_general(a, b, (((1,), (1,)), ((), ())), preferred_element_type=F32)


def dot_tn(a, b):
    return lax.dot_general(a, b, (((0,), (0,)), ((), ())), preferred_element_type=F32)


def gelu_only(z):
    t = jnp.tanh(z * (GELU_A + (GELU_A * GELU_B) * (z * z)))
    return z * (0.5 * t + 0.5)


def gelu_and_slope(z):
    s = (GELU_A * GELU_B) * (z * z)
    cdf = 0.5 * jnp.tanh(z * (GELU_A + s)) + 0.5
    a = z * cdf
    return a, cdf + (a * (1.0 - cdf)) * (2.0 * GELU_A + 6.0 * s)


def pick_block(size, target):
    block = min(size, target)
    while size % block:
        block //= 2
    return block


def loop(lo, hi, fn):
    def body(i, _):
        fn(i)
        return 0
    lax.fori_loop(lo, hi, body, 0)


def head_units(s, micros):
    return jnp.minimum(jnp.maximum(s - 1, 0), 3 * micros // 8)


def head_arrivals(s, stages, micros):
    return jnp.where(s == stages - 1, micros, head_units(s + 1, micros))


def signal_all(targets):
    sem = pltpu.get_barrier_semaphore()
    for target in targets:
        pl.semaphore_signal(sem, inc=1, device_id=target, device_id_type=MESH)
    pl.semaphore_wait(sem, len(targets))


def slices(size, block):
    return [slice(b * block, (b + 1) * block) for b in range(size // block)]


def act_pass(h, wi, a, slope, fb):
    for cols in slices(wi.shape[1], fb):
        act, der = gelu_and_slope(dot(h[...], wi[:, cols]))
        a[:, cols] = act.astype(BF16)
        slope[:, cols] = der


def front_kernel(stages, levels, micros, chunks, x_hbm, g_hbm, wi_hbm, wo_hbm, hall, y_out, eall, gin_hbm, gout_hbm, aup, qup, aqlow, elow,
                 wi, wo, hbuf, obuf, ebuf, gin, gout, abuf, qbuf, slope,
                 w_sem, x_sem, g_sem, f_send, f_recv, b_send, b_recv, y_sem, h_save, h_send, h_recv, e_save, e_send, e_recv,
                 a_save, a_load, o_sem, l_save):
    s = lax.axis_index('stage')
    d = lax.axis_index('data')
    nxt, prv = lax.rem(s + 1, stages), lax.rem(s + stages - 1, stages)
    up, down = lax.rem(d + 1, levels), lax.rem(d + levels - 1, levels)
    _, dim, hid = wi.shape
    tokens = hbuf.shape[1]
    half = tokens // 2
    nb = dim // chunks
    fb = pick_block(hid, 768)
    wb = pick_block(hid, 512)
    first = s == 0
    last = s == stages - 1
    inner = jnp.logical_not(last)
    lag = jnp.minimum(3 * (stages - 1 - s), micros)
    defer = s >= stages - 2
    heads, arrivals = head_units(s, micros), head_arrivals(s, stages, micros)

    def w_copies(v):
        return (pltpu.make_async_copy(wi_hbm.at[v], wi.at[v], w_sem.at[v, 0]),
                pltpu.make_async_copy(wo_hbm.at[v], wo.at[v], w_sem.at[v, 1]))

    def x_copy(m):
        return pltpu.make_async_copy(x_hbm.at[m], hbuf.at[m], x_sem.at[m])

    def g_copy(m):
        return pltpu.make_async_copy(g_hbm.at[m], ebuf.at[m], g_sem.at[m])

    def f_hop(i, slot, cols=slice(None)):
        return pltpu.make_async_remote_copy(
            src_ref=obuf.at[lax.rem(i, micros), :, cols], dst_ref=hbuf.at[slot, :, cols], send_sem=f_send.at[i], recv_sem=f_recv.at[slot],
            device_id={'stage': nxt}, device_id_type=MESH)

    def b_hop(m, cols=slice(None)):
        return pltpu.make_async_remote_copy(
            src_ref=obuf.at[lax.rem(m, micros), :, cols], dst_ref=ebuf.at[m, :, cols], send_sem=b_send.at[m], recv_sem=b_recv.at[m],
            device_id={'stage': prv}, device_id_type=MESH)

    def entry(m, cols=slice(None)):
        return pltpu.make_async_remote_copy(
            src_ref=obuf.at[m, :, cols], dst_ref=ebuf.at[micros + m, :, cols], send_sem=b_send.at[m], recv_sem=b_recv.at[micros + m],
            device_id={'stage': prv}, device_id_type=MESH)

    def low_keep(k):
        return (pltpu.make_async_copy(abuf.at[0], aqlow.at[k, 0], l_save.at[0]), pltpu.make_async_copy(qbuf.at[0], aqlow.at[k, 1], l_save.at[1]))

    def e_low_keep(k):
        return pltpu.make_async_copy(ebuf.at[micros + k], elow.at[k], l_save.at[2 + k])

    def y_copy(m):
        return pltpu.make_async_copy(obuf.at[m], y_out.at[m], y_sem.at[m])

    def h_keep(m):
        return pltpu.make_async_copy(hbuf.at[m], hall.at[m], h_save.at[m])

    def h_push(m, j):
        return pltpu.make_async_remote_copy(
            src_ref=hbuf.at[m], dst_ref=hall.at[(2 - j) * micros + m], send_sem=h_send.at[j, m], recv_sem=h_recv.at[1 - j, m],
            device_id={'data': (up, down)[j]}, device_id_type=MESH)

    def h_forward(m, j):
        rows = (slice(0, half), slice(half, tokens))[j]
        return pltpu.make_async_remote_copy(
            src_ref=hall.at[(2 - j) * micros + m, rows], dst_ref=hall.at[3 * micros + m, rows], send_sem=h_send.at[2 + j, m],
            recv_sem=h_recv.at[2, m], device_id={'data': (up, down)[j]}, device_id_type=MESH)

    def h_whole(m):
        return pltpu.make_async_remote_copy(
            src_ref=hall.at[m], dst_ref=hall.at[3 * micros + m], send_sem=h_send.at[2, m], recv_sem=h_recv.at[2, m],
            device_id={'data': up}, device_id_type=MESH)

    def e_keep(m):
        return pltpu.make_async_copy(obuf.at[m], eall.at[m], e_save.at[m])

    def e_push(m, j, cols=slice(None)):
        return pltpu.make_async_remote_copy(
            src_ref=obuf.at[m, :, cols], dst_ref=eall.at[(2 - j) * micros + m, :, cols], send_sem=e_send.at[j, m], recv_sem=e_recv.at[1 - j, m],
            device_id={'data': (up, down)[j]}, device_id_type=MESH)

    def e_forward(m, j):
        rows = (slice(0, half), slice(half, tokens))[j]
        return pltpu.make_async_remote_copy(
            src_ref=eall.at[(2 - j) * micros + m, rows], dst_ref=eall.at[3 * micros + m, rows], send_sem=e_send.at[2 + j, m],
            recv_sem=e_recv.at[2, m], device_id={'data': (up, down)[j]}, device_id_type=MESH)

    def e_whole(m):
        return pltpu.make_async_remote_copy(
            src_ref=eall.at[m], dst_ref=eall.at[3 * micros + m], send_sem=e_send.at[2, m], recv_sem=e_recv.at[2, m],
            device_id={'data': up}, device_id_type=MESH)

    def a_keep(m):
        return pltpu.make_async_copy(abuf.at[lax.rem(m, 2)], aup.at[m], a_save.at[0, m])

    def q_keep(m):
        return pltpu.make_async_copy(qbuf.at[lax.rem(m, 2)], qup.at[m], a_save.at[1, m])

    def loads(m):
        return (pltpu.make_async_copy(aup.at[m], abuf.at[1], a_load.at[0]), pltpu.make_async_copy(qup.at[m], qbuf.at[1], a_load.at[1]))

    outs = (pltpu.make_async_copy(gin, gin_hbm, o_sem.at[0]), pltpu.make_async_copy(gout, gout_hbm, o_sem.at[1]))

    for v in range(2):
        for c in w_copies(v):
            c.start()

    @pl.when(first)
    def _():
        loop(0, micros, lambda m: x_copy(m).start())

    @pl.when(last)
    def _():
        loop(0, micros, lambda m: g_copy(m).start())

    signal_all([{'stage': lax.rem(s + step, stages)} for step in range(1, stages)] + [{'data': up}, {'data': down}])

    w_copies(0)[0].wait()

    def fwd_wait(i):
        lower = i < micros

        @pl.when(first & lower)
        def _():
            x_copy(i).wait()

        @pl.when(jnp.logical_not(first & lower))
        def _():
            f_hop(i, i).wait_recv()

    def fwd_unit(i, aslot):
        v = i // micros
        lower = i < micros
        upper = jnp.logical_not(lower)
        o = lax.rem(i, micros)
        slot = jnp.where(last, i + micros, i)
        final = last & upper
        a = abuf.at[aslot]

        @pl.when(lower)
        def _():
            h_keep(i).start()
            h_push(i, 0).start()
            h_push(i, 1).start()

        @pl.when(upper)
        def _():
            f_hop(o, o).wait_send()
            h_push(o, 0).wait_recv()
            h_push(o, 1).wait_recv()
            h_forward(o, 0).start()
            h_forward(o, 1).start()

        @pl.when(jnp.logical_not(final))
        def _():
            for cols in slices(hid, fb):
                a[:, cols] = gelu_only(dot(hbuf[i], wi[v, :, cols])).astype(BF16)

        @pl.when(i == 0)
        def _():
            w_copies(0)[1].wait()

        for cols in slices(dim, nb):
            out = hbuf[i, :, cols].astype(F32) + dot(a[...], wo[v, :, cols])
            obuf[o, :, cols] = out.astype(BF16)

            @pl.when(jnp.logical_not(final))
            def _():
                f_hop(i, slot, cols).start()

        @pl.when(final)
        def _():
            y_copy(o).start()

    def bwd_unit(m, v, slot):
        q = qbuf.at[slot]
        upper = m < micros
        o = lax.rem(m, micros)

        @pl.when(last & upper)
        def _():
            g_copy(m).wait()
            y_copy(m).wait()

        @pl.when(jnp.logical_not(last & upper))
        def _():
            b_hop(m).wait_recv()

        @pl.when(inner & upper)
        def _():
            f_hop(micros + m, micros + m).wait_send()

        @pl.when(defer & upper & (m >= 2))
        def _():
            q_keep(m - 2).wait()

        @pl.when(jnp.logical_not(upper))
        def _():
            b_hop(o).wait_send()
            e_low_keep(o).start()

        for cols in slices(hid, fb):
            q[:, cols] = (slope[:, cols] * dot_nt(ebuf[m], wo[v, cols, :])).astype(BF16)
        for cols in slices(dim, nb):
            out = ebuf[m, :, cols].astype(F32) + dot_nt(q[...], wi[v, cols, :])
            obuf[o, :, cols] = out.astype(BF16)

            @pl.when(jnp.logical_not(first))
            def _():
                b_hop(m, cols).start()

            @pl.when(first)
            def _():
                entry(m, cols).start()
                e_push(m, 0, cols).start()
                e_push(m, 1, cols).start()

        @pl.when(first)
        def _():
            e_keep(m).start()

            @pl.when(m >= 1)
            def _():
                far(m - 1)

        @pl.when(defer & upper)
        def _():
            q_keep(m).start()

        @pl.when(jnp.logical_not(upper))
        def _():
            for c in low_keep(o):
                c.start()

    def far(m):
        for j in range(2):
            e_push(m, j).wait_recv()
        for j in range(2):
            e_forward(m, j).start()

    def weight_unit(m, k):
        for cols in slices(hid, wb):
            gin[:, cols] += dot_tn(hbuf[micros + m], qbuf[k, :, cols])

        @pl.when(m == micros - 1)
        def _():
            outs[0].start()

        for cols in slices(hid, wb):
            gout[cols, :] += dot_tn(abuf[k, :, cols], ebuf[m])

    def step(t):
        m = t - micros - lag
        low = m - micros
        upper = (m >= 0) & (low < 0)
        active = (m >= 0) & (low < heads)
        v = jnp.where(low < 0, 1, 0)
        slot = jnp.where(low < 0, lax.rem(t + micros + lag, 2), 0)
        w = jnp.where(defer, low, m)

        @pl.when(t == micros)
        def _():
            gin[...] = jnp.zeros_like(gin)
            gout[...] = jnp.zeros_like(gout)
            for c in w_copies(1):
                c.wait()

        @pl.when(defer & (low == 0))
        def _():
            for n in range(micros - 2, micros):
                a_keep(n).wait()
                q_keep(n).wait()

        @pl.when(defer & (low >= 0))
        def _():
            for c in loads(low):
                c.start()

        early = last & upper

        @pl.when(early)
        def _():
            fwd_wait(t)

        @pl.when(active)
        def _():
            @pl.when(defer & upper & (m >= 2))
            def _():
                a_keep(m - 2).wait()

            @pl.when(low >= 1)
            def _():
                for c in low_keep(low - 1):
                    c.wait()

            act_pass(hbuf.at[jnp.where(low < 0, micros + m, low)], wi.at[v], abuf.at[slot], slope, fb)

            @pl.when(defer & upper)
            def _():
                a_keep(m).start()

        @pl.when(t < 2 * micros)
        def _():
            @pl.when(jnp.logical_not(early))
            def _():
                fwd_wait(t)

            fwd_unit(t, jnp.where(early, slot, 2))

        @pl.when(active)
        def _():
            bwd_unit(m, v, slot)

        @pl.when(defer & (low >= 0))
        def _():
            for c in loads(low):
                c.wait()

        @pl.when((w >= 0) & (w < micros))
        def _():
            weight_unit(w, jnp.where(defer, 1, slot))

    loop(0, 2 * micros + lag + jnp.where(defer, micros, heads), step)

    outs[1].start()

    def drain(m):
        h_keep(m).wait()
        h_push(m, 0).wait_send()
        h_push(m, 1).wait_send()
        h_forward(m, 0).wait_send()
        h_forward(m, 1).wait_send()
        h_whole(m).wait_recv()

        @pl.when(jnp.logical_not(first) & (m >= heads))
        def _():
            b_hop(m).wait_send()

        @pl.when(m < heads)
        def _():
            b_hop(micros + m).wait_send()

        @pl.when((m >= heads) & (m < arrivals))
        def _():
            b_hop(micros + m).wait_recv()
            e_low_keep(m).start()

        @pl.when(m < arrivals)
        def _():
            e_low_keep(m).wait()

        @pl.when(first)
        def _():
            entry(m).wait_send()
            e_keep(m).wait()
            for j in range(2):
                e_push(m, j).wait_send()

            @pl.when(m < micros - 1)
            def _():
                e_whole(m).wait_recv()
                for j in range(2):
                    e_forward(m, j).wait_send()

            @pl.when(m == micros - 1)
            def _():
                for j in range(2):
                    e_push(m, j).wait_recv()

    loop(0, micros, drain)

    @pl.when(heads > 0)
    def _():
        for c in low_keep(heads - 1):
            c.wait()

    for c in outs:
        c.wait()


def run_front(stages, levels, x, g, w_in, w_out):
    micros, tokens, dim = x.shape
    _, _, hid = w_in.shape
    chunks = 3 if dim % 384 == 0 else 1
    dma = pltpu.SemaphoreType.DMA

    def rows(n):
        return jax.ShapeDtypeStruct((n * micros, tokens, dim), BF16)

    def acts(n):
        return jax.ShapeDtypeStruct((n * micros, tokens, hid), BF16)

    return pl.pallas_call(
        functools.partial(front_kernel, stages, levels, micros, chunks),
        out_shape=(rows(4), rows(1), rows(4), jax.ShapeDtypeStruct((dim, hid), F32), jax.ShapeDtypeStruct((hid, dim), F32),
                   acts(1), acts(1), jax.ShapeDtypeStruct((levels * micros, 2, tokens, hid), BF16), rows(levels)),
        in_specs=[ANY] * 4, out_specs=(ANY,) * 9,
        scratch_shapes=[
            pltpu.VMEM((2, dim, hid), BF16), pltpu.VMEM((2, hid, dim), BF16),
            pltpu.VMEM((2 * micros, tokens, dim), BF16), pltpu.VMEM((micros, tokens, dim), BF16), pltpu.VMEM((2 * micros, tokens, dim), BF16),
            pltpu.VMEM((dim, hid), F32), pltpu.VMEM((hid, dim), F32),
            pltpu.VMEM((3, tokens, hid), BF16), pltpu.VMEM((2, tokens, hid), BF16), pltpu.VMEM((tokens, hid), F32),
            dma((2, 2)), dma((micros,)), dma((micros,)), dma((2 * micros,)), dma((2 * micros,)), dma((2 * micros,)), dma((2 * micros,)), dma((micros,)),
            dma((micros,)), dma((4, micros)), dma((3, micros)), dma((micros,)), dma((4, micros)), dma((3, micros)),
            dma((2, micros)), dma((2,)), dma((2,)), dma((2 + micros,)),
        ],
        compiler_params=pltpu.CompilerParams(collective_id=0, has_side_effects=True, vmem_limit_bytes=VMEM_LIMIT),
        cost_estimate=pl.CostEstimate(flops=micros * 18 * tokens * dim * hid, bytes_accessed=4 * micros * tokens * hid * 2,
                                      transcendentals=3 * micros * tokens * hid),
        name='front',
    )(x, g, w_in, w_out)


def wide_kernel(stages, levels, micros, hall, eall, _y, _aq, _e, wi_hbm, wo_hbm, aq_out, e_out, dx_out, y_out,
                wi, wo, hbuf, obuf, ebuf, nbuf, aqbuf,
                w_sem, h_sem, n_send, b_send, b_recv, dx_sem, dx_send, dx_recv, y_send, y_recv, s_sem, k_sem, l_sem, n_sem, d_sem):
    s = lax.axis_index('stage')
    d = lax.axis_index('data')
    nxt, prv = lax.rem(s + 1, stages), lax.rem(s + stages - 1, stages)
    across = lax.rem(d + 2, levels)
    dim, hid = wi.shape
    units = ebuf.shape[0]
    fb = pick_block(hid, 768)
    ob = pick_block(dim, 256)
    groups = units // micros
    first = s == 0
    last = s == stages - 1
    heads, arrivals = head_units(s, micros), head_arrivals(s, stages, micros)

    w_copies = (pltpu.make_async_copy(wi_hbm.at[0], wi, w_sem.at[0]), pltpu.make_async_copy(wo_hbm.at[0], wo, w_sem.at[1]))

    def part(k):
        return pl.ds(k * micros, micros)

    def h_copy(k):
        return pltpu.make_async_copy(hall.at[part(k)], hbuf.at[part(k)], h_sem.at[k])

    def e_part(k):
        return pltpu.make_async_copy(ebuf.at[part(k)], e_out.at[part(k)], k_sem.at[k])

    def e_keep(i):
        return pltpu.make_async_copy(ebuf.at[i], e_out.at[i], l_sem.at[i])

    def n_load(k):
        return pltpu.make_async_copy(eall.at[part(k)], nbuf.at[part(k - 1)], n_sem.at[k - 1])

    def entry(i):
        return pltpu.make_async_remote_copy(
            src_ref=nbuf.at[i - micros], dst_ref=ebuf.at[i], send_sem=n_send.at[i - micros], recv_sem=b_recv.at[i],
            device_id={'stage': prv}, device_id_type=MESH)

    def entry_across():
        return pltpu.make_async_remote_copy(
            src_ref=eall.at[micros - 1], dst_ref=ebuf.at[units - 1], send_sem=d_sem, recv_sem=b_recv.at[units - 1],
            device_id={'stage': prv, 'data': across}, device_id_type=MESH)

    def b_hop(i):
        o = lax.rem(i, micros)
        return pltpu.make_async_remote_copy(
            src_ref=obuf.at[o], dst_ref=ebuf.at[i], send_sem=b_send.at[o], recv_sem=b_recv.at[i],
            device_id={'stage': prv}, device_id_type=MESH)

    def dx_copy(m):
        return pltpu.make_async_copy(obuf.at[m], dx_out.at[m], dx_sem.at[m])

    def dx_hop(m, src):
        return pltpu.make_async_remote_copy(
            src_ref=src.at[m], dst_ref=dx_out.at[m], send_sem=dx_send.at[m], recv_sem=dx_recv.at[m],
            device_id={'stage': nxt}, device_id_type=MESH)

    def y_hop(m):
        return pltpu.make_async_remote_copy(
            src_ref=y_out.at[m], dst_ref=y_out.at[m], send_sem=y_send.at[m], recv_sem=y_recv.at[m],
            device_id={'stage': nxt}, device_id_type=MESH)

    def e_load(i):
        return pltpu.make_async_copy(e_out.at[i], ebuf.at[i], l_sem.at[i])

    def relay(i):
        my = jnp.where(last, i, i - 2 - 2 * s)
        mx = i - 1 - 2 * s

        @pl.when((my >= 0) & (my < micros))
        def _():
            @pl.when(jnp.logical_not(last))
            def _():
                y_hop(my).wait_recv()

            @pl.when(s != stages - 2)
            def _():
                y_hop(my).start()

        @pl.when((mx >= 0) & (mx < micros) & jnp.logical_not(first))
        def _():
            dx_hop(mx, dx_out).wait_recv()

            @pl.when(jnp.logical_not(last))
            def _():
                dx_hop(mx, dx_out).start()

    def keep(i):
        k = lax.rem(i, 2)
        return pltpu.make_async_copy(aqbuf.at[k], aq_out.at[i], s_sem.at[k])

    for c in w_copies:
        c.start()
    for k in range(groups):
        h_copy(k).start()
    loop(heads, arrivals, lambda i: e_load(i).start())

    @pl.when(first)
    def _():
        for k in range(1, groups):
            n_load(k).start()

    signal_all([{'stage': lax.rem(s + step, stages)} for step in range(1, stages)]
               + [{'stage': st, 'data': across} for st in (nxt, prv)])

    @pl.when(first)
    def _():
        entry_across().start()
        for k in range(1, groups):
            n_load(k).wait()
            loop(k * micros, min((k + 1) * micros, units - 1), lambda i: entry(i).start())

    for c in w_copies:
        c.wait()

    def unit(i):
        k = lax.rem(i, 2)
        a, q = aqbuf.at[k, 0], aqbuf.at[k, 1]
        o = lax.rem(i, micros)

        @pl.when((o == 0) | (i == heads))
        def _():
            h_copy(i // micros).wait()

        @pl.when(i < arrivals)
        def _():
            e_load(i).wait()

        @pl.when(i >= arrivals)
        def _():
            b_hop(i).wait_recv()

        @pl.when(i >= heads + 2)
        def _():
            keep(i - 2).wait()

        relay(i - heads)

        for cols in slices(hid, fb):
            act, der = gelu_and_slope(dot(hbuf[i], wi[:, cols]))
            a[:, cols] = act.astype(BF16)
            q[:, cols] = (der * dot_nt(ebuf[i], wo[cols, :])).astype(BF16)

        keep(i).start()

        @pl.when(jnp.logical_not(first) & (i >= heads + micros))
        def _():
            b_hop(i - micros).wait_send()

        @pl.when(jnp.logical_not(first) | (i < micros))
        def _():
            for cols in slices(dim, ob):
                out = ebuf[i, :, cols].astype(F32) + dot_nt(q[...], wi[cols, :])
                obuf[o, :, cols] = out.astype(BF16)

            @pl.when(jnp.logical_not(first))
            def _():
                b_hop(i).start()

        @pl.when(first & (i < micros))
        def _():
            dx_copy(i).start()
            dx_hop(i, obuf).start()

        @pl.when((i >= arrivals) & (i < micros))
        def _():
            e_keep(i).start()

        @pl.when((o == micros - 1) & (i >= micros))
        def _():
            e_part(i // micros).start()

    loop(heads, units, unit)
    loop(units - heads, jnp.maximum(units - heads, micros + 2 * stages - 1), relay)

    @pl.when(first)
    def _():
        loop(micros, units - 1, lambda i: entry(i).wait_send())
        entry_across().wait_send()
        loop(0, micros, lambda m: dx_copy(m).wait())

    @pl.when(jnp.logical_not(first))
    def _():
        loop(units - micros, units, lambda i: b_hop(i).wait_send())

    @pl.when(jnp.logical_not(last))
    def _():
        loop(0, micros, lambda m: dx_hop(m, dx_out).wait_send())

    @pl.when(s != stages - 2)
    def _():
        loop(0, micros, lambda m: y_hop(m).wait_send())

    for i in (units - 2, units - 1):
        keep(i).wait()
    loop(arrivals, micros, lambda i: e_keep(i).wait())
    for k in range(1, groups):
        e_part(k).wait()


def run_wide(stages, levels, micros, hall, eall, y, aqlow, elow, w_in, w_out):
    units, tokens, dim = hall.shape
    _, _, hid = w_in.shape
    groups = units // micros
    dma = pltpu.SemaphoreType.DMA
    small = jax.ShapeDtypeStruct((micros, tokens, dim), BF16)
    acts = jax.ShapeDtypeStruct((units, 2, tokens, hid), BF16)
    return pl.pallas_call(
        functools.partial(wide_kernel, stages, levels, micros),
        out_shape=(acts, jax.ShapeDtypeStruct((units, tokens, dim), BF16), small, small),
        in_specs=[ANY] * 7, out_specs=(ANY,) * 4,
        scratch_shapes=[
            pltpu.VMEM((dim, hid), BF16), pltpu.VMEM((hid, dim), BF16),
            pltpu.VMEM((units, tokens, dim), BF16), pltpu.VMEM((micros, tokens, dim), BF16), pltpu.VMEM((units, tokens, dim), BF16),
            pltpu.VMEM((units - micros, tokens, dim), BF16), pltpu.VMEM((2, 2, tokens, hid), BF16),
            dma((2,)), dma((groups,)), dma((units - micros,)), dma((micros,)), dma((units,)), dma((micros,)), dma((micros,)), dma((micros,)),
            dma((micros,)), dma((micros,)), dma((2,)), dma((groups,)), dma((micros,)), dma((groups - 1,)), dma,
        ],
        input_output_aliases={2: 3, 3: 0, 4: 1},
        compiler_params=pltpu.CompilerParams(collective_id=1, has_side_effects=True, vmem_limit_bytes=VMEM_LIMIT),
        cost_estimate=pl.CostEstimate(flops=units * 6 * tokens * dim * hid, bytes_accessed=units * tokens * hid * 4,
                                      transcendentals=units * tokens * hid),
        name='wide',
    )(hall, eall, y, aqlow, elow, w_in, w_out)


def wgrad_kernel(lhs, rhs, *refs):
    others = (len(refs) - 1) // 2
    out = refs[others]

    @pl.when(pl.program_id(1) == 0)
    def _():
        out[...] = jnp.zeros_like(out)

    for src, dst in zip(refs[:others], refs[others + 1:]):
        dst[...] = src[...]
    lhs, rhs = (ref[...].reshape(-1, ref.shape[-1]) for ref in (lhs, rhs))
    out[0] += dot_tn(lhs, rhs)


def run_wgrad(rows, aq, which, split_lhs, others, name):
    units, tokens, dim = rows.shape
    hid = aq.shape[-1]
    ub = pick_block(units, max(1, 2048 // tokens))
    fb = pick_block(hid, 1024)
    grid = (hid // fb, units // ub)
    rows_spec = pl.BlockSpec((ub, tokens, dim), lambda j, k: (k, 0, 0))
    aq_spec = pl.BlockSpec((ub, None, tokens, fb), lambda j, k: (k, which, 0, j))
    if split_lhs:
        operands, specs = [aq, rows], [aq_spec, rows_spec]
        shape, out_spec = (2, hid, dim), pl.BlockSpec((1, fb, dim), lambda j, k: (0, j, 0))
    else:
        operands, specs = [rows, aq], [rows_spec, aq_spec]
        shape, out_spec = (2, dim, hid), pl.BlockSpec((1, dim, fb), lambda j, k: (0, 0, j))
    out_shapes, out_specs = [jax.ShapeDtypeStruct(shape, F32)], [out_spec]
    for other in others:
        count = pick_block(other.shape[0], grid[0] * grid[1])
        spec = pl.BlockSpec((other.shape[0] // count,) + other.shape[1:],
                            lambda j, k, count=count: (jnp.minimum(j * grid[1] + k, count - 1), 0, 0))
        operands.append(other)
        specs.append(spec)
        out_shapes.append(jax.ShapeDtypeStruct(other.shape, other.dtype))
        out_specs.append(spec)
    return pl.pallas_call(
        wgrad_kernel, grid=grid, out_shape=tuple(out_shapes), in_specs=specs, out_specs=tuple(out_specs),
        compiler_params=pltpu.CompilerParams(vmem_limit_bytes=VMEM_LIMIT),
        cost_estimate=pl.CostEstimate(flops=2 * units * tokens * dim * hid, bytes_accessed=2 * units * tokens * (dim + hid) + 4 * dim * hid,
                                      transcendentals=0),
        name=name,
    )(*operands)


def solution(mesh):
    stages, levels = mesh.shape['stage'], mesh.shape['data']

    def local_fn(x, g, w_in, w_out):
        wi, wo = w_in[:, 0], w_out[:, 0]
        hall, y, eall, gin_up, gout_up, _, _, aqlow, elow = run_front(stages, levels, x, g, wi, wo)
        gin_up, gout_up = lax.psum((gin_up, gout_up), 'data')
        aqlow, elow, dx, y = run_wide(stages, levels, x.shape[0], hall, eall, y, aqlow, elow, wi, wo)
        grad_in, dx, y = run_wgrad(hall, aqlow, 1, False, (dx, y), 'gin_low')
        grad_out, = run_wgrad(elow, aqlow, 0, True, (), 'gout_low')
        grad_in = lax.dynamic_update_slice(grad_in, gin_up[None], (1, 0, 0))
        grad_out = lax.dynamic_update_slice(grad_out, gout_up[None], (1, 0, 0))
        return y, dx, grad_in[:, None], grad_out[:, None]

    spec_rows = P(('part', 'data'))
    spec_weights = P(None, 'stage')
    spec_grads = P('part', 'stage')
    return jax.shard_map(local_fn, mesh=mesh, in_specs=(spec_rows, spec_rows, spec_weights, spec_weights), out_specs=(spec_rows, spec_rows, spec_grads, spec_grads), check_vma=False)
```
